256 devices in a mesh: groups: 2 (over y), tp: 16 (over z), tq: 4 (over x), tr: 2 (over core).
Axes of the slice: x: 4, y: 2, z: 16, core: 2. Of those that a mesh axis runs over, the one named last changes fastest.
The devices are a block of a 4x16x16 slice.
Arguments:
- attn_heads: bfloat16 [128, 16384], P('groups', ('tp', 'tq', 'tr')), parts along dimension 0, may hold values from -6 to 6
- residual: bfloat16 [128, 16384], P('groups', ('tp', 'tq', 'tr')), parts along dimension 0, may hold values from -120 to 120
- o_weight: bfloat16 [16384, 16384], P(('tp', 'tq', 'tr')), may hold values from -0.1875 to 0.1875
- norm_gain: bfloat16 [16384], P(('tp', 'tq', 'tr')), may hold values from 0.099609375 to 1.8984375
- q_weight: bfloat16 [16384, 16384], P(None, ('tp', 'tq', 'tr')), may hold values from -0.046875 to 0.046875
Outputs:
- hidden: bfloat16 [128, 16384], P('groups', ('tp', 'tq', 'tr')), parts along dimension 0
- peak_value: float32 [128], P('groups'), parts along dimension 0
- query: bfloat16 [128, 16384], P('groups', ('tp', 'tq', 'tr')), parts along dimension 0
The draws below stay inside these ranges and needn't reach their ends.
There are 2 independent parts, one for each index of `groups`. The reference program is written for one: setup_inputs(seed, part) draws one part's arguments, and reference() takes and returns one part's arrays. A program takes and returns all parts, laid end to end along the dimension named above; an argument that names none is the same for every part. Nothing has to cross between parts.
All inputs are finite; a program needn't handle non-finite values. Where the reference program divides by a largest or mean magnitude, that divisor is 1e-20 or more.
Results may differ from the reference program's by a relative error of at most 0.0095.
Values may be sent and summed in bfloat16 or wider, within the bound.
No kernel may reach another device: no remote copies, remote signals or barrier semaphores. Data moves between devices by JAX's collectives and lax.ppermute only.
A program may use at most 64 MiB of HBM per device.

```python
import jax
import jax.numpy as jnp
from jax import lax

D = 16384
TOK = 64
QD = 16384


def draw_residual(key, part):
    keys = jax.random.split(jax.random.fold_in(key, 11), 3)
    row_scale = jnp.exp(jax.random.uniform(keys[0], (TOK, 1), jnp.float32) * jnp.log(10.0))
    col_random = jnp.exp(jax.random.uniform(keys[1], (1, D), jnp.float32, jnp.log(0.5), jnp.log(5.0)))
    col_rise = jnp.exp(jnp.arange(D, dtype=jnp.float32)[None, :] / D * jnp.log(3.0))
    base_values = jax.random.normal(keys[2], (TOK, D), jnp.float32)
    base_values = jnp.clip(base_values, -4.0, 4.0)
    return (0.2 * base_values * row_scale * col_random * col_rise).astype(jnp.bfloat16)


def with_spikes(result, rng, source, target, blocks, factor):
    def block_of(axis_at):
        return (jnp.arange(result.shape[axis_at]) // (result.shape[axis_at] // blocks)).reshape((-1,) + (1,) * (result.ndim - 1 - axis_at))

    first = jax.random.permutation(rng, blocks)[block_of(target)]
    second = (block_of(target) + blocks // 2) % blocks
    return jnp.where((block_of(source) == first) | (block_of(source) == second), factor * result, result)


def shard_levels(key, shape, pieces, smallest, largest):
    level, own = 1.0, jax.random.fold_in(key, 6)
    for dim, blocks in pieces:
        steps = jnp.exp(jax.random.uniform(jax.random.fold_in(own, dim), (blocks,), jnp.float32, smallest / len(pieces), largest / len(pieces)))
        level = level * jnp.repeat(steps, shape[dim] // blocks).reshape([-1 if axis == dim else 1 for axis in range(len(shape))])
    return level


def normal_values(own_key, extent, spread, limit, shards=(), held_as=jnp.bfloat16):
    drawn = spread * jax.random.normal(own_key, extent, jnp.float32)
    if shards:
        drawn = drawn * shard_levels(own_key, extent, shards, -0.22, 0.18)
    return jnp.clip(drawn, -limit, limit).astype(held_as)


def heavy_noise(rng, extent, scale, most, shards, heavy, kind=jnp.bfloat16):
    result = scale * jax.random.normal(rng, extent, jnp.float32)
    if shards:
        result = result * shard_levels(rng, extent, shards, -0.22, 0.18)
    return jnp.clip(with_spikes(result, jax.random.fold_in(rng, 3), *heavy), -most, most).astype(kind)


def setup_inputs(seed: int = 0, part: int = 0) -> dict:
    seeds = jax.random.split(jax.random.key(seed), 6)
    part_keys = jax.random.split(jax.random.fold_in(seeds[5], part), 6)
    return {
        "attn_heads": normal_values(part_keys[0], (TOK, QD), 1.0, 6.0, ((1, 128),)),
        "residual": draw_residual(jax.random.fold_in(jax.random.fold_in(seeds[5], part), 71), part),
        "o_weight": heavy_noise(seeds[2], (QD, D), QD ** -0.5, 0.1875, ((0, 128),), (0, 1, 128, 5.5)),
        "norm_gain": jnp.clip(1.0 + 0.18 * jax.random.normal(seeds[3], (D,), jnp.float32), 0.099609375, 1.8984375).astype(jnp.bfloat16),
        "q_weight": normal_values(seeds[4], (D, QD), D ** -0.5, 0.046875, ((1, 128),)),
    }


def reference(attn_heads, residual, o_weight, norm_gain, q_weight):
    attn_total = jnp.dot(attn_heads, o_weight, preferred_element_type=jnp.float32)
    hidden = (residual.astype(jnp.float32) + attn_total).astype(jnp.bfloat16)
    widened = hidden.astype(jnp.float32)
    inv_rms = lax.rsqrt(lax.optimization_barrier(jnp.sum(widened * widened, axis=1)) / D + 1e-05)
    normed = widened * norm_gain.astype(jnp.float32) * inv_rms[:, None]
    peak_value = lax.optimization_barrier(jnp.max(jnp.abs(normed), axis=1))
    quantized = (normed * (448.0 / (peak_value + 1e-06))[:, None]).astype(jnp.bfloat16)
    projected = jnp.dot(quantized, q_weight, preferred_element_type=jnp.float32)
    query = (projected * ((peak_value + 1e-06) / 448.0)[:, None]).astype(jnp.bfloat16)
    return (hidden, peak_value, query)
```

```python
import functools

import jax
import jax.numpy as jnp
from jax import lax
from jax.experimental import pallas as pl
from jax.experimental.pallas import tpu as pltpu
from jax.sharding import PartitionSpec as P

EPS = 1e-05
TINY = 1e-06
TOP = 448.0
BF16, F32 = jnp.bfloat16, jnp.float32
STAT_ROWS = 8
VMEM = pl.BlockSpec(memory_space=pltpu.VMEM)
SMEM = pl.BlockSpec(memory_space=pltpu.SMEM)
ANY = pl.BlockSpec(memory_space=pl.ANY)


def params(mib):
    return pltpu.CompilerParams(vmem_limit_bytes=mib << 20)


def cost(flops, moved):
    return pl.CostEstimate(flops=flops, bytes_accessed=moved, transcendentals=0)


def project_kernel(dims, core_ref, heads_ref, weight_ref, out_ref, held, sems):
    tp, tq, tr, width = dims
    core = core_ref[0]

    def copy(q, t):
        source = pl.multiple_of(((t * tq + q) * tr + core) * width, width)
        place = q * tp + t
        return pltpu.make_async_copy(
            weight_ref.at[:, pl.ds(source, width)],
            held.at[:, pl.ds(pl.multiple_of(place * width, width), width)],
            sems.at[place],
        )

    for q in range(tq):
        for t in range(tp):
            copy(q, t).start()
    heads = heads_ref[...]
    group = 4
    for q in range(tq):
        for t in range(0, tp, group):
            for k in range(group):
                copy(q, t + k).wait()
            at = (q * tp + t) * width
            terms = jnp.dot(heads, held[:, at : at + group * width], preferred_element_type=F32)
            for k in range(group):
                out_ref[q, t + k] = terms[:, k * width : (k + 1) * width].astype(out_ref.dtype)


def project(core, heads, weight, dims, kind):
    tp, tq, tr, width = dims
    tokens, depth = heads.shape
    blocks = tp * tq
    return pl.pallas_call(
        functools.partial(project_kernel, dims),
        out_shape=jax.ShapeDtypeStruct((tq, tp, tokens, width), kind),
        in_specs=[SMEM, VMEM, ANY],
        out_specs=VMEM,
        scratch_shapes=[
            pltpu.VMEM((depth, blocks * width), BF16),
            pltpu.SemaphoreType.DMA((blocks,)),
        ],
        compiler_params=params(16),
        cost_estimate=cost(2 * tokens * depth * blocks * width, 2 * depth * blocks * width),
        name="project",
    )(core, heads, weight)


def joined_kernel(mine_ref, other_ref, out_ref):
    for q in range(mine_ref.shape[0]):
        out_ref[q] = (mine_ref[q] + other_ref[q].astype(F32)).astype(BF16)


def joined(mine, other):
    return pl.pallas_call(
        joined_kernel,
        out_shape=jax.ShapeDtypeStruct(mine.shape, BF16),
        in_specs=[VMEM, VMEM],
        out_specs=VMEM,
        compiler_params=params(16),
        cost_estimate=cost(mine.size, 8 * mine.size),
        name="joined",
    )(mine, other)


def summed_kernel(parts_ref, out_ref):
    total = parts_ref[0].astype(F32)
    for k in range(1, parts_ref.shape[0]):
        total = total + parts_ref[k].astype(F32)
    out_ref[...] = total.astype(BF16)


def summed(parts):
    return pl.pallas_call(
        summed_kernel,
        out_shape=jax.ShapeDtypeStruct(parts.shape[1:], BF16),
        in_specs=[VMEM],
        out_specs=VMEM,
        compiler_params=params(16),
        cost_estimate=cost(parts.size, 4 * parts.size),
        name="summed",
    )(parts)


def in_three(value):
    first = value.astype(BF16)
    rest = value - first.astype(F32)
    second = rest.astype(BF16)
    third = (rest - second.astype(F32)).astype(BF16)
    return [first.astype(F32), second.astype(F32), third.astype(F32)]


def normed_kernel(parts_ref, residual_ref, gain_ref, hidden_ref, sent_ref):
    total = parts_ref[0].astype(F32)
    for k in range(1, parts_ref.shape[0]):
        total = total + parts_ref[k].astype(F32)
    hidden = (residual_ref[...].astype(F32) + total).astype(BF16)
    hidden_ref[...] = hidden
    widened = hidden.astype(F32)
    gained = widened * gain_ref[...].astype(F32)
    tokens, width = gained.shape
    blank = jnp.zeros((width - tokens, width), F32)

    def turned(rows):
        return jnp.transpose(jnp.concatenate([rows, blank], axis=0))

    squares = jnp.sum(turned(widened * widened), axis=0, keepdims=True)
    top = jnp.max(turned(jnp.abs(gained)), axis=0, keepdims=True)
    lines = in_three(squares) + in_three(top)
    lines.append(jnp.zeros((STAT_ROWS - len(lines), width), F32))
    block = jnp.concatenate([gained] + lines, axis=0).astype(BF16)
    for k in range(sent_ref.shape[0]):
        sent_ref[k] = block


def normed(parts, residual, gain):
    copies, tokens, width = parts.shape
    return pl.pallas_call(
        normed_kernel,
        out_shape=(
            jax.ShapeDtypeStruct((tokens, width), BF16),
            jax.ShapeDtypeStruct((copies, tokens + STAT_ROWS, width), BF16),
        ),
        in_specs=[VMEM, VMEM, VMEM],
        out_specs=(VMEM, VMEM),
        compiler_params=params(16),
        cost_estimate=cost(parts.size, 4 * parts.size),
        name="normed",
    )(parts, residual, gain)


def query_sum(core, dims, tokens, found_ref, weight_ref, held, sems):
    tp, tq, tr, width = dims

    def copy(q, t):
        source = pl.multiple_of(((t * tq + q) * tr + core) * width, width)
        place = q * tp + t
        return pltpu.make_async_copy(
            weight_ref.at[pl.ds(source, width), :],
            held.at[pl.ds(place * width, width), :],
            sems.at[place],
        )

    for q in range(tq):
        for t in range(tp):
            copy(q, t).start()
    total = None
    group = 4
    for q in range(tq):
        for t in range(0, tp, group):
            for k in range(group):
                copy(q, t + k).wait()
            left = jnp.concatenate(
                [found_ref[q, t + k, 0:tokens, :] for k in range(group)], axis=1
            )
            at = (q * tp + t) * width
            term = jnp.dot(left, held[at : at + group * width, :], preferred_element_type=F32)
            total = term if total is None else total + term
    return total


def query_half_kernel(dims, core_ref, found_ref, weight_ref, out_ref, held, sems):
    out_ref[...] = query_sum(core_ref[0], dims, out_ref.shape[0], found_ref, weight_ref, held, sems)


def query_half(core, found, weight, dims, tokens):
    tp, tq, tr, width = dims
    depth = tp * tq * width
    return pl.pallas_call(
        functools.partial(query_half_kernel, dims),
        out_shape=jax.ShapeDtypeStruct((tokens, width), F32),
        in_specs=[SMEM, VMEM, ANY],
        out_specs=VMEM,
        scratch_shapes=[
            pltpu.VMEM((depth, width), BF16),
            pltpu.SemaphoreType.DMA((tp * tq,)),
        ],
        compiler_params=params(16),
        cost_estimate=cost(2 * tokens * depth * width, 2 * depth * width),
        name="query_half",
    )(core, found, weight)


def query_kernel(dims, features, core_ref, part_ref, mine_ref, other_ref, weight_ref, query_ref, peak_ref, held, sems):
    tokens, width = query_ref.shape
    total = part_ref[...] + query_sum(
        core_ref[0], dims, tokens, other_ref, weight_ref, held, sems
    )
    squares, top = None, None
    for ref in (mine_ref, other_ref):
        for q in range(dims[1]):
            for t in range(dims[0]):
                lines = ref[q, t, tokens : tokens + STAT_ROWS, :].astype(F32)
                found = (lines[0:1] + lines[1:2]) + lines[2:3]
                largest = (lines[3:4] + lines[4:5]) + lines[5:6]
                squares = found if squares is None else squares + found
                top = largest if top is None else jnp.maximum(top, largest)
    inv_rms = lax.rsqrt(squares / features + EPS)
    peak = top * inv_rms
    peak_ref[...] = peak[:, 0:tokens]
    scale = inv_rms * (TOP / (peak + TINY)) * ((peak + TINY) / TOP)
    column = jnp.transpose(jnp.broadcast_to(scale, (width, width)))
    query_ref[...] = (total * column[0:tokens, :]).astype(BF16)


def query_rest(core, part, mine, other, weight, dims, features):
    tp, tq, tr, width = dims
    tokens = part.shape[0]
    depth = tp * tq * width
    return pl.pallas_call(
        functools.partial(query_kernel, dims, features),
        out_shape=(
            jax.ShapeDtypeStruct((tokens, width), BF16),
            jax.ShapeDtypeStruct((1, tokens), F32),
        ),
        in_specs=[SMEM, VMEM, VMEM, VMEM, ANY],
        out_specs=(VMEM, VMEM),
        scratch_shapes=[
            pltpu.VMEM((depth, width), BF16),
            pltpu.SemaphoreType.DMA((tp * tq,)),
        ],
        compiler_params=params(16),
        cost_estimate=cost(2 * tokens * depth * width, 2 * depth * width),
        name="query_rest",
    )(core, part, mine, other, weight)


def exchanged(blocks, axis):
    return lax.all_to_all(blocks, axis, split_axis=0, concat_axis=0, tiled=True)


def swapped(array):
    return lax.ppermute(array, "tr", [(0, 1), (1, 0)])


def body(attn_heads, residual, o_weight, norm_gain, q_weight):
    tp, tq, tr = (lax.axis_size(axis) for axis in ("tp", "tq", "tr"))
    tokens, width = residual.shape
    features = o_weight.shape[1]
    dims = (tp, tq, tr, width)
    core = lax.axis_index("tr").astype(jnp.int32).reshape(1)
    other_core = 1 - core

    sent = project(other_core, attn_heads, o_weight, dims, BF16)
    arrived = swapped(sent)
    mine = project(core, attn_heads, o_weight, dims, F32)
    section = joined(mine, arrived).reshape(tq, tp * tokens, width)
    section = summed(exchanged(section, "tq")).reshape(tp, tokens, width)
    hidden, block = normed(exchanged(section, "tp"), residual, norm_gain.reshape(1, width))

    rows = tokens + STAT_ROWS
    line = exchanged(block, "tp").reshape(tp * rows, width)
    plane = exchanged(jnp.broadcast_to(line, (tq, *line.shape)), "tq").reshape(tq, tp, rows, width)
    other_plane = swapped(plane)
    part = query_half(core, plane, q_weight, dims, tokens)
    query, peak = query_rest(other_core, part, plane, other_plane, q_weight, dims, features)
    return hidden, peak.reshape(tokens), query


def solution(mesh):
    split = ("tp", "tq", "tr")
    placed = (P("groups", split), P("groups", split), P(split, None), P(split), P(None, split))
    return jax.shard_map(
        body,
        mesh=mesh,
        in_specs=placed,
        out_specs=(P("groups", split), P("groups"), P("groups", split)),
        check_vma=False,
    )
```

```python
import functools

import jax
import jax.numpy as jnp
from jax import lax
from jax.experimental import pallas as pl
from jax.experimental.pallas import tpu as pltpu
from jax.sharding import PartitionSpec as P

EPS = 1e-05
TINY = 1e-06
TOP = 448.0
BF16, F32 = jnp.bfloat16, jnp.float32
STAT_ROWS = 8
VMEM = pl.BlockSpec(memory_space=pltpu.VMEM)
SMEM = pl.BlockSpec(memory_space=pltpu.SMEM)
ANY = pl.BlockSpec(memory_space=pl.ANY)


def params(mib):
    return pltpu.CompilerParams(vmem_limit_bytes=mib << 20)


def cost(flops, moved):
    return pl.CostEstimate(flops=flops, bytes_accessed=moved, transcendentals=0)


def project_kernel(dims, core_ref, heads_ref, weight_ref, out_ref):
    tp, tq, tr, width = dims
    core = core_ref[0]
    heads = heads_ref[...]
    for t in range(tp):
        starts = [pl.multiple_of(((t * tq + q) * tr + core) * width, width) for q in range(tq)]
        weight = jnp.concatenate([weight_ref[:, pl.ds(at, width)] for at in starts], axis=1)
        terms = jnp.dot(heads, weight, preferred_element_type=F32)
        for q in range(tq):
            out_ref[q, t] = terms[:, q * width : (q + 1) * width].astype(out_ref.dtype)


def project(core, heads, weight, dims, kind):
    tp, tq, tr, width = dims
    tokens, depth = heads.shape
    return pl.pallas_call(
        functools.partial(project_kernel, dims),
        out_shape=jax.ShapeDtypeStruct((tq, tp, tokens, width), kind),
        in_specs=[SMEM, VMEM, VMEM],
        out_specs=VMEM,
        compiler_params=params(16),
        cost_estimate=cost(tokens * weight.size, 2 * weight.size),
        name="project",
    )(core, heads, weight)


def joined_kernel(mine_ref, other_ref, out_ref):
    for q in range(mine_ref.shape[0]):
        out_ref[q] = (mine_ref[q] + other_ref[q].astype(F32)).astype(BF16)


def joined(mine, other):
    return pl.pallas_call(
        joined_kernel,
        out_shape=jax.ShapeDtypeStruct(mine.shape, BF16),
        in_specs=[VMEM, VMEM],
        out_specs=VMEM,
        compiler_params=params(16),
        cost_estimate=cost(mine.size, 8 * mine.size),
        name="joined",
    )(mine, other)


def summed_kernel(parts_ref, out_ref):
    total = parts_ref[0].astype(F32)
    for k in range(1, parts_ref.shape[0]):
        total = total + parts_ref[k].astype(F32)
    out_ref[...] = total.astype(BF16)


def summed(parts):
    return pl.pallas_call(
        summed_kernel,
        out_shape=jax.ShapeDtypeStruct(parts.shape[1:], BF16),
        in_specs=[VMEM],
        out_specs=VMEM,
        compiler_params=params(16),
        cost_estimate=cost(parts.size, 4 * parts.size),
        name="summed",
    )(parts)


def in_three(value):
    first = value.astype(BF16)
    rest = value - first.astype(F32)
    second = rest.astype(BF16)
    third = (rest - second.astype(F32)).astype(BF16)
    return [first.astype(F32), second.astype(F32), third.astype(F32)]


def normed_kernel(parts_ref, residual_ref, gain_ref, hidden_ref, sent_ref):
    total = parts_ref[0].astype(F32)
    for k in range(1, parts_ref.shape[0]):
        total = total + parts_ref[k].astype(F32)
    hidden = (residual_ref[...].astype(F32) + total).astype(BF16)
    hidden_ref[...] = hidden
    widened = hidden.astype(F32)
    gained = widened * gain_ref[...].astype(F32)
    tokens, width = gained.shape
    blank = jnp.zeros((width - tokens, width), F32)

    def turned(rows):
        return jnp.transpose(jnp.concatenate([rows, blank], axis=0))

    squares = jnp.sum(turned(widened * widened), axis=0, keepdims=True)
    top = jnp.max(turned(jnp.abs(gained)), axis=0, keepdims=True)
    lines = in_three(squares) + in_three(top)
    lines.append(jnp.zeros((STAT_ROWS - len(lines), width), F32))
    block = jnp.concatenate([gained] + lines, axis=0).astype(BF16)
    for k in range(sent_ref.shape[0]):
        sent_ref[k] = block


def normed(parts, residual, gain):
    copies, tokens, width = parts.shape
    return pl.pallas_call(
        normed_kernel,
        out_shape=(
            jax.ShapeDtypeStruct((tokens, width), BF16),
            jax.ShapeDtypeStruct((copies, tokens + STAT_ROWS, width), BF16),
        ),
        in_specs=[VMEM, VMEM, VMEM],
        out_specs=(VMEM, VMEM),
        compiler_params=params(16),
        cost_estimate=cost(parts.size, 4 * parts.size),
        name="normed",
    )(parts, residual, gain)


def query_sum(core, dims, tokens, found_ref, weight_ref):
    tp, tq, tr, width = dims
    group = 4
    total = None
    for q in range(tq):
        for t in range(0, tp, group):
            turns = [t + k for k in range(min(group, tp - t))]
            starts = [pl.multiple_of(((k * tq + q) * tr + core) * width, width) for k in turns]
            left = jnp.concatenate([found_ref[q, k, 0:tokens, :] for k in turns], axis=1)
            right = jnp.concatenate([weight_ref[pl.ds(at, width), :] for at in starts], axis=0)
            term = jnp.dot(left, right, preferred_element_type=F32)
            total = term if total is None else total + term
    return total


def stat_lines(ref, dims, tokens):
    squares, top = None, None
    for q in range(dims[1]):
        for t in range(dims[0]):
            lines = ref[q, t, tokens : tokens + STAT_ROWS, :].astype(F32)
            found = (lines[0:1] + lines[1:2]) + lines[2:3]
            largest = (lines[3:4] + lines[4:5]) + lines[5:6]
            squares = found if squares is None else squares + found
            top = largest if top is None else jnp.maximum(top, largest)
    return squares, top


def query_half_kernel(dims, core_ref, found_ref, weight_ref, part_ref, stat_ref):
    tokens = part_ref.shape[0]
    part_ref[...] = query_sum(core_ref[0], dims, tokens, found_ref, weight_ref)
    squares, top = stat_lines(found_ref, dims, tokens)
    stat_ref[0:1, :] = squares
    stat_ref[1:2, :] = top


def query_half(core, found, weight, dims, tokens):
    width = dims[3]
    return pl.pallas_call(
        functools.partial(query_half_kernel, dims),
        out_shape=(
            jax.ShapeDtypeStruct((tokens, width), F32),
            jax.ShapeDtypeStruct((2, width), F32),
        ),
        in_specs=[SMEM, VMEM, VMEM],
        out_specs=(VMEM, VMEM),
        compiler_params=params(16),
        cost_estimate=cost(tokens * weight.size, weight.size),
        name="query_half",
    )(core, found, weight)


def query_kernel(dims, features, core_ref, part_ref, stat_ref, found_ref, weight_ref, query_ref, peak_ref):
    tokens, width = query_ref.shape
    total = part_ref[...] + query_sum(core_ref[0], dims, tokens, found_ref, weight_ref)
    squares, top = stat_lines(found_ref, dims, tokens)
    squares = squares + stat_ref[0:1, :]
    top = jnp.maximum(top, stat_ref[1:2, :])
    inv_rms = lax.rsqrt(squares / features + EPS)
    peak = top * inv_rms
    peak_ref[...] = peak[:, 0:tokens]
    scale = inv_rms * (TOP / (peak + TINY)) * ((peak + TINY) / TOP)
    column = jnp.transpose(jnp.broadcast_to(scale, (width, width)))
    query_ref[...] = (total * column[0:tokens, :]).astype(BF16)


def query_rest(core, part, stats, found, weight, dims, features):
    tokens, width = part.shape
    return pl.pallas_call(
        functools.partial(query_kernel, dims, features),
        out_shape=(
            jax.ShapeDtypeStruct((tokens, width), BF16),
            jax.ShapeDtypeStruct((1, tokens), F32),
        ),
        in_specs=[SMEM, VMEM, VMEM, VMEM, VMEM],
        out_specs=(VMEM, VMEM),
        compiler_params=params(16),
        cost_estimate=cost(tokens * weight.size, weight.size),
        name="query_rest",
    )(core, part, stats, found, weight)


def exchanged(blocks, axis):
    return lax.all_to_all(blocks, axis, split_axis=0, concat_axis=0, tiled=True)


def swapped(array):
    return lax.ppermute(array, "tr", [(0, 1), (1, 0)])


def body(attn_heads, residual, o_weight, norm_gain, q_weight):
    tp, tq, tr = (lax.axis_size(axis) for axis in ("tp", "tq", "tr"))
    tokens, width = residual.shape
    features = o_weight.shape[1]
    dims = (tp, tq, tr, width)
    core = lax.axis_index("tr").astype(jnp.int32).reshape(1)
    other_core = 1 - core

    sent = project(other_core, attn_heads, o_weight, dims, BF16)
    arrived = swapped(sent)
    mine = project(core, attn_heads, o_weight, dims, F32)
    section = joined(mine, arrived).reshape(tq, tp * tokens, width)
    section = summed(exchanged(section, "tq")).reshape(tp, tokens, width)
    hidden, block = normed(exchanged(section, "tp"), residual, norm_gain.reshape(1, width))

    rows = tokens + STAT_ROWS
    line = exchanged(block, "tp").reshape(tp * rows, width)
    plane = exchanged(jnp.broadcast_to(line, (tq, *line.shape)), "tq").reshape(tq, tp, rows, width)
    other_plane = swapped(plane)
    part, stats = query_half(core, plane, q_weight, dims, tokens)
    query, peak = query_rest(other_core, part, stats, other_plane, q_weight, dims, features)
    return hidden, peak.reshape(tokens), query


def solution(mesh):
    split = ("tp", "tq", "tr")
    placed = (P("groups", split), P("groups", split), P(split, None), P(split), P(None, split))
    return jax.shard_map(
        body,
        mesh=mesh,
        in_specs=placed,
        out_specs=(P("groups", split), P("groups"), P("groups", split)),
        check_vma=False,
    )
```

```python
import functools

import jax
import jax.numpy as jnp
from jax import lax
from jax.experimental import pallas as pl
from jax.experimental.pallas import tpu as pltpu
from jax.sharding import PartitionSpec as P

EPS = 1e-05
TINY = 1e-06
TOP = 448.0
BF16, F32 = jnp.bfloat16, jnp.float32
STAT_ROWS = 8
NEAR = (1, -1, 0)
VMEM = pl.BlockSpec(memory_space=pltpu.VMEM)
SMEM = pl.BlockSpec(memory_space=pltpu.SMEM)
ANY = pl.BlockSpec(memory_space=pl.ANY)


def params(mib):
    return pltpu.CompilerParams(vmem_limit_bytes=mib << 20)


def cost(flops, moved):
    return pl.CostEstimate(flops=flops, bytes_accessed=moved, transcendentals=0)


def project_kernel(dims, place_ref, heads_ref, weight_ref, far_ref, near_ref):
    tp, tq, tr, width = dims
    core, here = place_ref[0], place_ref[1]
    heads = heads_ref[...]
    steps = [tq // 2] + [k for k in NEAR]
    for t in range(tp):
        starts = []
        for step in steps:
            q = lax.rem(here + (step + tq), tq)
            starts.append(pl.multiple_of(((t * tq + q) * tr + core) * width, width))
        weight = jnp.concatenate([weight_ref[:, pl.ds(at, width)] for at in starts], axis=1)
        terms = jnp.dot(heads, weight, preferred_element_type=F32)
        far_ref[t] = terms[:, 0:width].astype(far_ref.dtype)
        for k in range(1, len(steps)):
            near_ref[k - 1, t] = terms[:, k * width : (k + 1) * width].astype(near_ref.dtype)


def project(place, heads, weight, dims, kind):
    tp, tq, tr, width = dims
    tokens, depth = heads.shape
    return pl.pallas_call(
        functools.partial(project_kernel, dims),
        out_shape=(
            jax.ShapeDtypeStruct((tp, tokens, width), kind),
            jax.ShapeDtypeStruct((len(NEAR), tp, tokens, width), kind),
        ),
        in_specs=[SMEM, VMEM, VMEM],
        out_specs=(VMEM, VMEM),
        compiler_params=params(16),
        cost_estimate=cost(tokens * weight.size, 2 * weight.size),
        name="project",
    )(place, heads, weight)


def far_kernel(mine_ref, other_ref, right_ref, left_ref):
    half = right_ref.shape[0]
    for k in range(half):
        right_ref[k] = (mine_ref[k] + other_ref[k].astype(F32)).astype(BF16)
        left_ref[k] = (mine_ref[half + k] + other_ref[half + k].astype(F32)).astype(BF16)


def far_block(mine, other):
    half = jax.ShapeDtypeStruct((mine.shape[0] // 2, *mine.shape[1:]), BF16)
    return pl.pallas_call(
        far_kernel,
        out_shape=(half, half),
        in_specs=[VMEM, VMEM],
        out_specs=(VMEM, VMEM),
        compiler_params=params(16),
        cost_estimate=cost(mine.size, 8 * mine.size),
        name="far_block",
    )(mine, other)


def near_kernel(mine_ref, other_ref, left_got_ref, right_got_ref, right_ref, left_ref, own_ref):
    half = left_got_ref.shape[0]
    for t in range(right_ref.shape[0]):
        right = mine_ref[0, t] + other_ref[0, t].astype(F32)
        left = mine_ref[1, t] + other_ref[1, t].astype(F32)
        if t < half:
            right = right + left_got_ref[t].astype(F32)
        else:
            left = left + right_got_ref[t - half].astype(F32)
        right_ref[t] = right.astype(BF16)
        left_ref[t] = left.astype(BF16)
        own_ref[t] = mine_ref[2, t] + other_ref[2, t].astype(F32)


def near_blocks(mine, other, left_got, right_got):
    shape = mine.shape[1:]
    block = jax.ShapeDtypeStruct(shape, BF16)
    return pl.pallas_call(
        near_kernel,
        out_shape=(block, block, jax.ShapeDtypeStruct(shape, F32)),
        in_specs=[VMEM] * 4,
        out_specs=(VMEM, VMEM, VMEM),
        compiler_params=params(16),
        cost_estimate=cost(mine.size, 8 * mine.size),
        name="near_blocks",
    )(mine, other, left_got, right_got)


def summed_kernel(own_ref, left_ref, right_ref, out_ref):
    for t in range(out_ref.shape[0]):
        total = own_ref[t] + left_ref[t].astype(F32) + right_ref[t].astype(F32)
        out_ref[t] = total.astype(BF16)


def summed(own, left, right):
    return pl.pallas_call(
        summed_kernel,
        out_shape=jax.ShapeDtypeStruct(own.shape, BF16),
        in_specs=[VMEM] * 3,
        out_specs=VMEM,
        compiler_params=params(16),
        cost_estimate=cost(2 * own.size, 8 * own.size),
        name="summed",
    )(own, left, right)


def in_three(value):
    first = value.astype(BF16)
    rest = value - first.astype(F32)
    second = rest.astype(BF16)
    third = (rest - second.astype(F32)).astype(BF16)
    return [first.astype(F32), second.astype(F32), third.astype(F32)]


def normed_kernel(parts_ref, residual_ref, gain_ref, hidden_ref, sent_ref):
    total = parts_ref[0].astype(F32)
    for k in range(1, parts_ref.shape[0]):
        total = total + parts_ref[k].astype(F32)
    hidden = (residual_ref[...].astype(F32) + total).astype(BF16)
    hidden_ref[...] = hidden
    widened = hidden.astype(F32)
    gained = widened * gain_ref[...].astype(F32)
    tokens, width = gained.shape
    blank = jnp.zeros((width - tokens, width), F32)

    def turned(rows):
        return jnp.transpose(jnp.concatenate([rows, blank], axis=0))

    squares = jnp.sum(turned(widened * widened), axis=0, keepdims=True)
    top = jnp.max(turned(jnp.abs(gained)), axis=0, keepdims=True)
    lines = in_three(squares) + in_three(top)
    lines.append(jnp.zeros((STAT_ROWS - len(lines), width), F32))
    block = jnp.concatenate([gained] + lines, axis=0).astype(BF16)
    for k in range(sent_ref.shape[0]):
        sent_ref[k] = block


def normed(parts, residual, gain):
    copies, tokens, width = parts.shape
    return pl.pallas_call(
        normed_kernel,
        out_shape=(
            jax.ShapeDtypeStruct((tokens, width), BF16),
            jax.ShapeDtypeStruct((copies, tokens + STAT_ROWS, width), BF16),
        ),
        in_specs=[VMEM, VMEM, VMEM],
        out_specs=(VMEM, VMEM),
        compiler_params=params(16),
        cost_estimate=cost(parts.size, 4 * parts.size),
        name="normed",
    )(parts, residual, gain)


def query_sum(dims, tokens, pieces, weight_ref):
    tp, tq, tr, width = dims
    group = 4
    total = None
    for ref, core, q, first in pieces:
        for t in range(0, ref.shape[0], group):
            turns = range(t, min(t + group, ref.shape[0]))
            starts = [
                pl.multiple_of((((first + k) * tq + q) * tr + core) * width, width) for k in turns
            ]
            left = jnp.concatenate([ref[k, 0:tokens, :] for k in turns], axis=1)
            right = jnp.concatenate([weight_ref[pl.ds(at, width), :] for at in starts], axis=0)
            term = jnp.dot(left, right, preferred_element_type=F32)
            total = term if total is None else total + term
    return total


def stat_lines(tokens, refs):
    squares, top = None, None
    for ref in refs:
        for t in range(ref.shape[0]):
            lines = ref[t, tokens : tokens + STAT_ROWS, :].astype(F32)
            found = (lines[0:1] + lines[1:2]) + lines[2:3]
            largest = (lines[3:4] + lines[4:5]) + lines[5:6]
            squares = found if squares is None else squares + found
            top = largest if top is None else jnp.maximum(top, largest)
    return squares, top


def around(dims, place_ref):
    tq = dims[1]
    core, here = place_ref[0], place_ref[1]
    return core, 1 - core, [lax.rem(here + (k + tq), tq) for k in (0, -1, 1, tq // 2)]


def query_near_kernel(dims, place_ref, *refs):
    *found, weight_ref, part_ref, stat_ref = refs
    tokens = part_ref.shape[0]
    core, other, at = around(dims, place_ref)
    pieces = [(ref, core, q, 0) for ref, q in zip(found[:3], at)]
    pieces += [(ref, other, q, 0) for ref, q in zip(found[3:], at)]
    part_ref[...] = query_sum(dims, tokens, pieces, weight_ref)
    squares, top = stat_lines(tokens, found)
    stat_ref[0:1, :] = squares
    stat_ref[1:2, :] = top


def query_near(place, found, weight, dims, tokens):
    width = dims[3]
    return pl.pallas_call(
        functools.partial(query_near_kernel, dims),
        out_shape=(
            jax.ShapeDtypeStruct((tokens, width), F32),
            jax.ShapeDtypeStruct((2, width), F32),
        ),
        in_specs=[SMEM] + [VMEM] * (len(found) + 1),
        out_specs=(VMEM, VMEM),
        compiler_params=params(16),
        cost_estimate=cost(tokens * weight.size, weight.size),
        name="query_near",
    )(place, *found, weight)


def query_far_kernel(dims, features, place_ref, part_ref, stat_ref, *refs):
    *found, weight_ref, query_ref, peak_ref = refs
    tokens, width = query_ref.shape
    core, other, at = around(dims, place_ref)
    half = dims[0] // 2
    pieces = [(found[k], (core, core, other, other)[k], at[3], (k % 2) * half) for k in range(4)]
    total = part_ref[...] + query_sum(dims, tokens, pieces, weight_ref)
    squares, top = stat_lines(tokens, found)
    squares = squares + stat_ref[0:1, :]
    top = jnp.maximum(top, stat_ref[1:2, :])
    inv_rms = lax.rsqrt(squares / features + EPS)
    peak = top * inv_rms
    peak_ref[...] = peak[:, 0:tokens]
    scale = inv_rms * (TOP / (peak + TINY)) * ((peak + TINY) / TOP)
    column = jnp.transpose(jnp.broadcast_to(scale, (width, width)))
    query_ref[...] = (total * column[0:tokens, :]).astype(BF16)


def query_far(place, part, stats, found, weight, dims, features):
    tokens, width = part.shape
    return pl.pallas_call(
        functools.partial(query_far_kernel, dims, features),
        out_shape=(
            jax.ShapeDtypeStruct((tokens, width), BF16),
            jax.ShapeDtypeStruct((1, tokens), F32),
        ),
        in_specs=[SMEM] + [VMEM] * (len(found) + 3),
        out_specs=(VMEM, VMEM),
        compiler_params=params(16),
        cost_estimate=cost(tokens * weight.size, weight.size),
        name="query_far",
    )(place, part, stats, *found, weight)


def exchanged(blocks, axis):
    return lax.all_to_all(blocks, axis, split_axis=0, concat_axis=0, tiled=True)


def swapped(array):
    return lax.ppermute(array, "tr", [(0, 1), (1, 0)])


def moved(array, step):
    size = lax.axis_size("tq")
    return lax.ppermute(array, "tq", [(k, (k + step) % size) for k in range(size)])


def body(attn_heads, residual, o_weight, norm_gain, q_weight):
    tp, tq, tr = (lax.axis_size(axis) for axis in ("tp", "tq", "tr"))
    tokens, width = residual.shape
    features = o_weight.shape[1]
    dims = (tp, tq, tr, width)
    core = lax.axis_index("tr").astype(jnp.int32)
    here = lax.axis_index("tq").astype(jnp.int32)
    place = jnp.stack([core, here])
    other_place = jnp.stack([1 - core, here])

    sent_far, sent_near = project(other_place, attn_heads, o_weight, dims, BF16)
    came_far, came_near = swapped(sent_far), swapped(sent_near)
    mine_far, mine_near = project(place, attn_heads, o_weight, dims, F32)
    far_right, far_left = far_block(mine_far, came_far)
    right, left, own = near_blocks(mine_near, came_near, moved(far_right, 1), moved(far_left, -1))
    section = summed(own, moved(right, 1), moved(left, -1))
    hidden, block = normed(exchanged(section, "tp"), residual, norm_gain.reshape(1, width))

    line = exchanged(block, "tp")
    from_left, from_right = moved(line, 1), moved(line, -1)
    half = tp // 2
    far_first = moved(from_left[:half], 1)
    far_last = moved(from_right[half:], -1)
    near = [line, from_left, from_right]
    far = [far_first, far_last]
    part, stats = query_near(place, near + [swapped(k) for k in near], q_weight, dims, tokens)
    query, peak = query_far(
        place, part, stats, far + [swapped(k) for k in far], q_weight, dims, features
    )
    return hidden, peak.reshape(tokens), query


def solution(mesh):
    split = ("tp", "tq", "tr")
    placed = (P("groups", split), P("groups", split), P(split, None), P(split), P(None, split))
    return jax.shard_map(
        body,
        mesh=mesh,
        in_specs=placed,
        out_specs=(P("groups", split), P("groups"), P("groups", split)),
        check_vma=False,
    )
```

```python
import functools

import jax
import jax.numpy as jnp
from jax import lax
from jax.experimental import pallas as pl
from jax.experimental.pallas import tpu as pltpu
from jax.sharding import PartitionSpec as P


EPS = 1e-05
TINY = 1e-06
TOP = 448.0
BF16, F32 = jnp.bfloat16, jnp.float32
STAT_ROWS = 8
NEAR = (1, -1, 0)
VMEM = pl.BlockSpec(memory_space=pltpu.VMEM)
SMEM = pl.BlockSpec(memory_space=pltpu.SMEM)
ANY = pl.BlockSpec(memory_space=pl.ANY)


def params(mib):
    return pltpu.CompilerParams(vmem_limit_bytes=mib << 20)


def cost(flops, moved):
    return pl.CostEstimate(flops=flops, bytes_accessed=moved, transcendentals=0)


def terms_kernel(dims, place_ref, heads_ref, weight_ref, far_sent_ref, far_mine_ref, near_sent_ref, near_mine_ref):
    tp, tq, tr, width = dims
    core, here = place_ref[0], place_ref[1]
    span = tr * width
    heads = heads_ref[...]
    for t in range(tp):
        for k, step in enumerate((tq // 2,) + NEAR):
            q = lax.rem(here + (step + tq), tq)
            columns = pl.ds(pl.multiple_of((t * tq + q) * span, span), span)
            terms = jnp.dot(heads, weight_ref[:, columns], preferred_element_type=F32)
            low, high = terms[:, 0:width], terms[:, width:span]
            mine = jnp.where(core == 0, low, high)
            sent = jnp.where(core == 0, high, low).astype(BF16)
            if k == 0:
                far_mine_ref[t] = mine
                far_sent_ref[t] = sent
            else:
                near_mine_ref[k - 1, t] = mine
                near_sent_ref[k - 1, t] = sent


def all_terms(place, heads, weight, dims):
    tp, _, _, width = dims
    tokens, _ = heads.shape
    far, near = (tp, tokens, width), (len(NEAR), tp, tokens, width)
    return pl.pallas_call(
        functools.partial(terms_kernel, dims),
        out_shape=(
            jax.ShapeDtypeStruct(far, BF16),
            jax.ShapeDtypeStruct(far, F32),
            jax.ShapeDtypeStruct(near, BF16),
            jax.ShapeDtypeStruct(near, F32),
        ),
        in_specs=[SMEM, VMEM, VMEM],
        out_specs=(VMEM,) * 4,
        compiler_params=params(16),
        cost_estimate=cost(2 * tokens * weight.size, 2 * weight.size),
        name="all_terms",
    )(place, heads, weight)


def far_kernel(mine_ref, other_ref, right_ref, left_ref):
    half = right_ref.shape[0]
    for k in range(half):
        right_ref[k] = (mine_ref[k] + other_ref[k].astype(F32)).astype(BF16)
        left_ref[k] = (mine_ref[half + k] + other_ref[half + k].astype(F32)).astype(BF16)


def far_block(mine, other):
    half = jax.ShapeDtypeStruct((mine.shape[0] // 2, *mine.shape[1:]), BF16)
    return pl.pallas_call(
        far_kernel,
        out_shape=(half, half),
        in_specs=[VMEM, VMEM],
        out_specs=(VMEM, VMEM),
        compiler_params=params(16),
        cost_estimate=cost(mine.size, 8 * mine.size),
        name="far_block",
    )(mine, other)


def near_kernel(mine_ref, other_ref, left_got_ref, right_got_ref, right_ref, left_ref, own_ref):
    half = left_got_ref.shape[0]
    for t in range(right_ref.shape[0]):
        right = mine_ref[0, t] + other_ref[0, t].astype(F32)
        left = mine_ref[1, t] + other_ref[1, t].astype(F32)
        if t < half:
            right = right + left_got_ref[t].astype(F32)
        else:
            left = left + right_got_ref[t - half].astype(F32)
        right_ref[t] = right.astype(BF16)
        left_ref[t] = left.astype(BF16)
        own_ref[t] = mine_ref[2, t] + other_ref[2, t].astype(F32)


def near_blocks(mine, other, left_got, right_got):
    shape = mine.shape[1:]
    block = jax.ShapeDtypeStruct(shape, BF16)
    return pl.pallas_call(
        near_kernel,
        out_shape=(block, block, jax.ShapeDtypeStruct(shape, F32)),
        in_specs=[VMEM] * 4,
        out_specs=(VMEM, VMEM, VMEM),
        compiler_params=params(16),
        cost_estimate=cost(mine.size, 8 * mine.size),
        name="near_blocks",
    )(mine, other, left_got, right_got)


def summed_kernel(own_ref, left_ref, right_ref, out_ref):
    for t in range(out_ref.shape[0]):
        total = own_ref[t] + left_ref[t].astype(F32) + right_ref[t].astype(F32)
        out_ref[t] = total.astype(BF16)


def summed(own, left, right):
    return pl.pallas_call(
        summed_kernel,
        out_shape=jax.ShapeDtypeStruct(own.shape, BF16),
        in_specs=[VMEM] * 3,
        out_specs=VMEM,
        compiler_params=params(16),
        cost_estimate=cost(2 * own.size, 8 * own.size),
        name="summed",
    )(own, left, right)


def in_three(value):
    first = value.astype(BF16)
    rest = value - first.astype(F32)
    second = rest.astype(BF16)
    third = (rest - second.astype(F32)).astype(BF16)
    return [first.astype(F32), second.astype(F32), third.astype(F32)]


def normed_kernel(parts_ref, residual_ref, gain_ref, hidden_ref, sent_ref):
    total = parts_ref[0].astype(F32)
    for k in range(1, parts_ref.shape[0]):
        total = total + parts_ref[k].astype(F32)
    hidden = (residual_ref[...].astype(F32) + total).astype(BF16)
    hidden_ref[...] = hidden
    widened = hidden.astype(F32)
    gained = widened * gain_ref[...].astype(F32)
    tokens, width = gained.shape
    blank = jnp.zeros((width - tokens, width), F32)

    def turned(rows):
        return jnp.transpose(jnp.concatenate([rows, blank], axis=0))

    squares = jnp.sum(turned(widened * widened), axis=0, keepdims=True)
    top = jnp.max(turned(jnp.abs(gained)), axis=0, keepdims=True)
    lines = in_three(squares) + in_three(top)
    lines.append(jnp.zeros((STAT_ROWS - len(lines), width), F32))
    block = jnp.concatenate([gained] + lines, axis=0).astype(BF16)
    for k in range(sent_ref.shape[0]):
        sent_ref[k] = block


def normed(parts, residual, gain):
    copies, tokens, width = parts.shape
    return pl.pallas_call(
        normed_kernel,
        out_shape=(
            jax.ShapeDtypeStruct((tokens, width), BF16),
            jax.ShapeDtypeStruct((copies, tokens + STAT_ROWS, width), BF16),
        ),
        in_specs=[VMEM, VMEM, VMEM],
        out_specs=(VMEM, VMEM),
        compiler_params=params(16),
        cost_estimate=cost(parts.size, 4 * parts.size),
        name="normed",
    )(parts, residual, gain)


def query_sum(core, dims, tokens, found_ref, weight_ref):
    tp, tq, tr, width = dims
    group = 4
    total = None
    for q in range(tq):
        for t in range(0, tp, group):
            turns = range(t, min(t + group, tp))
            starts = [pl.multiple_of(((k * tq + q) * tr + core) * width, width) for k in turns]
            left = jnp.concatenate(
                [found_ref[q, k * tokens : (k + 1) * tokens, :] for k in turns], axis=1
            )
            right = jnp.concatenate([weight_ref[pl.ds(at, width), :] for at in starts], axis=0)
            term = jnp.dot(left, right, preferred_element_type=F32)
            total = term if total is None else total + term
    return total


def stat_lines(blocks):
    squares, top = None, None
    for block in blocks:
        lines = block.astype(F32)
        found = (lines[0:1] + lines[1:2]) + lines[2:3]
        largest = (lines[3:4] + lines[4:5]) + lines[5:6]
        squares = found if squares is None else squares + found
        top = largest if top is None else jnp.maximum(top, largest)
    return squares, top


def plane_stats(found_ref):
    rows = found_ref.shape[1]
    return stat_lines([found_ref[q, rows - STAT_ROWS :, :] for q in range(found_ref.shape[0])])


def query_kernel(dims, features, core_ref, mine_ref, other_ref, weight_ref, query_ref, peak_ref):
    tokens, width = query_ref.shape
    core = core_ref[0]
    squares, top = plane_stats(mine_ref)
    other_squares, other_top = plane_stats(other_ref)
    squares = squares + other_squares
    top = jnp.maximum(top, other_top)
    inv_rms = lax.rsqrt(squares / features + EPS)
    peak = top * inv_rms
    peak_ref[...] = peak[:, 0:tokens]
    scale = inv_rms * (TOP / (peak + TINY)) * ((peak + TINY) / TOP)
    column = jnp.transpose(jnp.broadcast_to(scale, (width, width)))
    total = query_sum(core, dims, tokens, mine_ref, weight_ref)
    total = total + query_sum(1 - core, dims, tokens, other_ref, weight_ref)
    query_ref[...] = (total * column[0:tokens, :]).astype(BF16)


def query_all(core, mine, other, weight, dims, tokens, features):
    width = dims[3]
    return pl.pallas_call(
        functools.partial(query_kernel, dims, features),
        out_shape=(
            jax.ShapeDtypeStruct((tokens, width), BF16),
            jax.ShapeDtypeStruct((1, tokens), F32),
        ),
        in_specs=[SMEM, VMEM, VMEM, VMEM],
        out_specs=(VMEM, VMEM),
        compiler_params=params(16),
        cost_estimate=cost(2 * tokens * weight.size, 2 * weight.size),
        name="query_all",
    )(core, mine, other, weight)


def restacked_kernel(line_ref, out_ref):
    tp, rows, width = line_ref.shape
    tokens = rows - STAT_ROWS
    squares, top = stat_lines([line_ref[t, tokens:rows, :] for t in range(tp)])
    lines = in_three(squares) + in_three(top)
    lines.append(jnp.zeros((STAT_ROWS - len(lines), width), F32))
    block = jnp.concatenate(lines, axis=0).astype(BF16)
    for k in range(out_ref.shape[0]):
        for t in range(tp):
            out_ref[k, t * tokens : (t + 1) * tokens, :] = line_ref[t, 0:tokens, :]
        out_ref[k, tp * tokens : tp * tokens + STAT_ROWS, :] = block


def restacked(line, copies):
    tp, rows, width = line.shape
    shape = (copies, tp * (rows - STAT_ROWS) + STAT_ROWS, width)
    return pl.pallas_call(
        restacked_kernel,
        out_shape=jax.ShapeDtypeStruct(shape, BF16),
        in_specs=[VMEM],
        out_specs=VMEM,
        compiler_params=params(16),
        cost_estimate=cost(line.size, 8 * line.size),
        name="restacked",
    )(line)


def exchanged(blocks, axis):
    return lax.all_to_all(blocks, axis, split_axis=0, concat_axis=0, tiled=True)


def swapped(array):
    return lax.ppermute(array, "tr", [(0, 1), (1, 0)])


def moved(array, step):
    size = lax.axis_size("tq")
    return lax.ppermute(array, "tq", [(k, (k + step) % size) for k in range(size)])


def step(attn_heads, residual, o_weight, norm_gain, q_weight):
    tp, tq, tr = (lax.axis_size(axis) for axis in ("tp", "tq", "tr"))
    tokens, width = residual.shape
    features = o_weight.shape[1]
    dims = (tp, tq, tr, width)
    core = lax.axis_index("tr").astype(jnp.int32)
    here = lax.axis_index("tq").astype(jnp.int32)
    place = jnp.stack([core, here])

    far_sent, far_mine, near_sent, near_mine = all_terms(place, attn_heads, o_weight, dims)
    far_right, far_left = far_block(far_mine, swapped(far_sent))
    near_came = swapped(near_sent)
    left_got, right_got = moved(far_right, 1), moved(far_left, -1)
    right, left, own = near_blocks(near_mine, near_came, left_got, right_got)
    section = summed(own, moved(right, 1), moved(left, -1))
    hidden, block = normed(exchanged(section, "tp"), residual, norm_gain.reshape(1, width))

    plane = exchanged(restacked(exchanged(block, "tp"), tq), "tq")
    other_plane = swapped(plane)
    query, peak = query_all(
        core.reshape(1), plane, other_plane, q_weight, dims, tokens, features
    )
    return hidden, peak.reshape(tokens), query


def solution(mesh):
    split = ("tp", "tq", "tr")
    placed = (P("groups", split), P("groups", split), P(split, None), P(split), P(None, split))
    return jax.shard_map(
        step,
        mesh=mesh,
        in_specs=placed,
        out_specs=(P("groups", split), P("groups"), P("groups", split)),
        check_vma=False,
    )
```

```python
import functools

import jax
import jax.numpy as jnp
from jax import lax
from jax.experimental import pallas as pl
from jax.experimental.pallas import tpu as pltpu
from jax.sharding import PartitionSpec as P


EPS = 1e-05
TINY = 1e-06
TOP = 448.0
BF16, F32 = jnp.bfloat16, jnp.float32
STAT_ROWS = 8
NEAR = (1, -1, 0)
VMEM = pl.BlockSpec(memory_space=pltpu.VMEM)
SMEM = pl.BlockSpec(memory_space=pltpu.SMEM)
ANY = pl.BlockSpec(memory_space=pl.ANY)


def params(mib):
    return pltpu.CompilerParams(vmem_limit_bytes=mib << 20)


def cost(flops, moved):
    return pl.CostEstimate(flops=flops, bytes_accessed=moved, transcendentals=0)


def terms_kernel(dims, place_ref, heads_ref, weight_ref, far_sent_ref, far_mine_ref, near_sent_ref, near_mine_ref):
    tp, tq, tr, width = dims
    core, here = place_ref[0], place_ref[1]
    span = tr * width
    heads = heads_ref[...]
    for t in range(tp):
        for k, step in enumerate((tq // 2,) + NEAR):
            q = lax.rem(here + (step + tq), tq)
            columns = pl.ds(pl.multiple_of((t * tq + q) * span, span), span)
            terms = jnp.dot(heads, weight_ref[:, columns], preferred_element_type=F32)
            low, high = terms[:, 0:width], terms[:, width:span]
            mine = jnp.where(core == 0, low, high)
            sent = jnp.where(core == 0, high, low).astype(BF16)
            if k == 0:
                far_mine_ref[t] = mine
                far_sent_ref[t] = sent
            else:
                near_mine_ref[k - 1, t] = mine
                near_sent_ref[k - 1, t] = sent


def all_terms(place, heads, weight, dims):
    tp, _, _, width = dims
    tokens, _ = heads.shape
    far, near = (tp, tokens, width), (len(NEAR), tp, tokens, width)
    return pl.pallas_call(
        functools.partial(terms_kernel, dims),
        out_shape=(
            jax.ShapeDtypeStruct(far, BF16),
            jax.ShapeDtypeStruct(far, F32),
            jax.ShapeDtypeStruct(near, BF16),
            jax.ShapeDtypeStruct(near, F32),
        ),
        in_specs=[SMEM, VMEM, VMEM],
        out_specs=(VMEM,) * 4,
        compiler_params=params(16),
        cost_estimate=cost(2 * tokens * weight.size, 2 * weight.size),
        name="all_terms",
    )(place, heads, weight)


def far_kernel(mine_ref, other_ref, right_ref, left_ref):
    half = right_ref.shape[0]
    for k in range(half):
        right_ref[k] = (mine_ref[k] + other_ref[k].astype(F32)).astype(BF16)
        left_ref[k] = (mine_ref[half + k] + other_ref[half + k].astype(F32)).astype(BF16)


def far_block(mine, other):
    half = jax.ShapeDtypeStruct((mine.shape[0] // 2, *mine.shape[1:]), BF16)
    return pl.pallas_call(
        far_kernel,
        out_shape=(half, half),
        in_specs=[VMEM, VMEM],
        out_specs=(VMEM, VMEM),
        compiler_params=params(16),
        cost_estimate=cost(mine.size, 8 * mine.size),
        name="far_block",
    )(mine, other)


def near_kernel(mine_ref, other_ref, left_got_ref, right_got_ref, right_ref, left_ref, own_ref):
    half = left_got_ref.shape[0]
    for t in range(right_ref.shape[0]):
        right = mine_ref[0, t] + other_ref[0, t].astype(F32)
        left = mine_ref[1, t] + other_ref[1, t].astype(F32)
        if t < half:
            right = right + left_got_ref[t].astype(F32)
        else:
            left = left + right_got_ref[t - half].astype(F32)
        right_ref[t] = right.astype(BF16)
        left_ref[t] = left.astype(BF16)
        own_ref[t] = mine_ref[2, t] + other_ref[2, t].astype(F32)


def near_blocks(mine, other, left_got, right_got):
    shape = mine.shape[1:]
    block = jax.ShapeDtypeStruct(shape, BF16)
    return pl.pallas_call(
        near_kernel,
        out_shape=(block, block, jax.ShapeDtypeStruct(shape, F32)),
        in_specs=[VMEM] * 4,
        out_specs=(VMEM, VMEM, VMEM),
        compiler_params=params(16),
        cost_estimate=cost(mine.size, 8 * mine.size),
        name="near_blocks",
    )(mine, other, left_got, right_got)


def summed_kernel(own_ref, left_ref, right_ref, out_ref):
    for t in range(out_ref.shape[0]):
        total = own_ref[t] + left_ref[t].astype(F32) + right_ref[t].astype(F32)
        out_ref[t] = total.astype(BF16)


def summed(own, left, right):
    return pl.pallas_call(
        summed_kernel,
        out_shape=jax.ShapeDtypeStruct(own.shape, BF16),
        in_specs=[VMEM] * 3,
        out_specs=VMEM,
        compiler_params=params(16),
        cost_estimate=cost(2 * own.size, 8 * own.size),
        name="summed",
    )(own, left, right)


def in_three(value):
    first = value.astype(BF16)
    rest = value - first.astype(F32)
    second = rest.astype(BF16)
    third = (rest - second.astype(F32)).astype(BF16)
    return [first.astype(F32), second.astype(F32), third.astype(F32)]


def normed_kernel(parts_ref, residual_ref, gain_ref, hidden_ref, sent_ref):
    total = parts_ref[0].astype(F32)
    for k in range(1, parts_ref.shape[0]):
        total = total + parts_ref[k].astype(F32)
    hidden = (residual_ref[...].astype(F32) + total).astype(BF16)
    hidden_ref[...] = hidden
    widened = hidden.astype(F32)
    gained = widened * gain_ref[...].astype(F32)
    tokens, width = gained.shape
    blank = jnp.zeros((width - tokens, width), F32)

    def turned(rows):
        return jnp.transpose(jnp.concatenate([rows, blank], axis=0))

    squares = jnp.sum(turned(widened * widened), axis=0, keepdims=True)
    top = jnp.max(turned(jnp.abs(gained)), axis=0, keepdims=True)
    lines = in_three(squares) + in_three(top)
    lines.append(jnp.zeros((STAT_ROWS - len(lines), width), F32))
    block = jnp.concatenate([gained] + lines, axis=0).astype(BF16)
    for k in range(sent_ref.shape[0]):
        sent_ref[k] = block


def normed(parts, residual, gain):
    copies, tokens, width = parts.shape
    return pl.pallas_call(
        normed_kernel,
        out_shape=(
            jax.ShapeDtypeStruct((tokens, width), BF16),
            jax.ShapeDtypeStruct((copies, tokens + STAT_ROWS, width), BF16),
        ),
        in_specs=[VMEM, VMEM, VMEM],
        out_specs=(VMEM, VMEM),
        compiler_params=params(16),
        cost_estimate=cost(parts.size, 4 * parts.size),
        name="normed",
    )(parts, residual, gain)


def query_sum(core, dims, tokens, found_ref, weight_ref):
    tp, tq, tr, width = dims
    group = 4
    total = None
    for q in range(tq):
        for t in range(0, tp, group):
            turns = range(t, min(t + group, tp))
            starts = [pl.multiple_of(((k * tq + q) * tr + core) * width, width) for k in turns]
            left = jnp.concatenate(
                [found_ref[q, k * tokens : (k + 1) * tokens, :] for k in turns], axis=1
            )
            right = jnp.concatenate([weight_ref[pl.ds(at, width), :] for at in starts], axis=0)
            term = jnp.dot(left, right, preferred_element_type=F32)
            total = term if total is None else total + term
    return total


def stat_lines(blocks):
    squares, top = None, None
    for block in blocks:
        lines = block.astype(F32)
        found = (lines[0:1] + lines[1:2]) + lines[2:3]
        largest = (lines[3:4] + lines[4:5]) + lines[5:6]
        squares = found if squares is None else squares + found
        top = largest if top is None else jnp.maximum(top, largest)
    return squares, top


def plane_stats(found_ref):
    rows = found_ref.shape[1]
    return stat_lines([found_ref[q, rows - STAT_ROWS :, :] for q in range(found_ref.shape[0])])


def query_kernel(dims, features, core_ref, mine_ref, other_ref, weight_ref, hidden_ref, query_ref, peak_ref, hidden_out_ref):
    tokens, width = query_ref.shape
    hidden_out_ref[...] = hidden_ref[...]
    core = core_ref[0]
    squares, top = plane_stats(mine_ref)
    other_squares, other_top = plane_stats(other_ref)
    squares = squares + other_squares
    top = jnp.maximum(top, other_top)
    inv_rms = lax.rsqrt(squares / features + EPS)
    peak = top * inv_rms
    peak_ref[...] = peak[:, 0:tokens]
    scale = inv_rms * (TOP / (peak + TINY)) * ((peak + TINY) / TOP)
    column = jnp.transpose(jnp.broadcast_to(scale, (width, width)))
    total = query_sum(core, dims, tokens, mine_ref, weight_ref)
    total = total + query_sum(1 - core, dims, tokens, other_ref, weight_ref)
    query_ref[...] = (total * column[0:tokens, :]).astype(BF16)


def query_all(core, mine, other, weight, hidden, dims, features):
    tokens, width = hidden.shape
    return pl.pallas_call(
        functools.partial(query_kernel, dims, features),
        out_shape=(
            jax.ShapeDtypeStruct((tokens, width), BF16),
            jax.ShapeDtypeStruct((1, tokens), F32),
            jax.ShapeDtypeStruct((tokens, width), BF16),
        ),
        in_specs=[SMEM, VMEM, VMEM, VMEM, VMEM],
        out_specs=(VMEM, VMEM, VMEM),
        compiler_params=params(16),
        cost_estimate=cost(2 * tokens * weight.size, 2 * weight.size),
        name="query_all",
    )(core, mine, other, weight, hidden)


def restacked_kernel(line_ref, out_ref):
    tp, rows, width = line_ref.shape
    tokens = rows - STAT_ROWS
    squares, top = stat_lines([line_ref[t, tokens:rows, :] for t in range(tp)])
    lines = in_three(squares) + in_three(top)
    lines.append(jnp.zeros((STAT_ROWS - len(lines), width), F32))
    block = jnp.concatenate(lines, axis=0).astype(BF16)
    for k in range(out_ref.shape[0]):
        for t in range(tp):
            out_ref[k, t * tokens : (t + 1) * tokens, :] = line_ref[t, 0:tokens, :]
        out_ref[k, tp * tokens : tp * tokens + STAT_ROWS, :] = block


def restacked(line, copies):
    tp, rows, width = line.shape
    shape = (copies, tp * (rows - STAT_ROWS) + STAT_ROWS, width)
    return pl.pallas_call(
        restacked_kernel,
        out_shape=jax.ShapeDtypeStruct(shape, BF16),
        in_specs=[VMEM],
        out_specs=VMEM,
        compiler_params=params(16),
        cost_estimate=cost(line.size, 8 * line.size),
        name="restacked",
    )(line)


def exchanged(blocks, axis):
    return lax.all_to_all(blocks, axis, split_axis=0, concat_axis=0, tiled=True)


def swapped(array):
    return lax.ppermute(array, "tr", [(0, 1), (1, 0)])


def moved(array, step):
    size = lax.axis_size("tq")
    return lax.ppermute(array, "tq", [(k, (k + step) % size) for k in range(size)])


def step(attn_heads, residual, o_weight, norm_gain, q_weight):
    tp, tq, tr = (lax.axis_size(axis) for axis in ("tp", "tq", "tr"))
    tokens, width = residual.shape
    features = o_weight.shape[1]
    dims = (tp, tq, tr, width)
    core = lax.axis_index("tr").astype(jnp.int32)
    here = lax.axis_index("tq").astype(jnp.int32)
    place = jnp.stack([core, here])

    far_sent, far_mine, near_sent, near_mine = all_terms(place, attn_heads, o_weight, dims)
    far_right, far_left = far_block(far_mine, swapped(far_sent))
    near_came = swapped(near_sent)
    left_got, right_got = moved(far_right, 1), moved(far_left, -1)
    right, left, own = near_blocks(near_mine, near_came, left_got, right_got)
    section = summed(own, moved(right, 1), moved(left, -1))
    hidden, block = normed(exchanged(section, "tp"), residual, norm_gain.reshape(1, width))

    plane = exchanged(restacked(exchanged(block, "tp"), tq), "tq")
    other_plane = swapped(plane)
    query, peak, hidden = query_all(
        core.reshape(1), plane, other_plane, q_weight, hidden, dims, features
    )
    return hidden, peak.reshape(tokens), query


def solution(mesh):
    split = ("tp", "tq", "tr")
    placed = (P("groups", split), P("groups", split), P(split, None), P(split), P(None, split))
    return jax.shard_map(
        step,
        mesh=mesh,
        in_specs=placed,
        out_specs=(P("groups", split), P("groups"), P("groups", split)),
        check_vma=False,
    )
```

```python
import functools

import jax
import jax.numpy as jnp
from jax import lax
from jax.experimental import pallas as pl
from jax.experimental.pallas import tpu as pltpu
from jax.sharding import PartitionSpec as P


EPS = 1e-05
TINY = 1e-06
TOP = 448.0
BF16, F32 = jnp.bfloat16, jnp.float32
STAT_ROWS = 8
NEAR = (1, -1, 0)
VMEM = pl.BlockSpec(memory_space=pltpu.VMEM)
SMEM = pl.BlockSpec(memory_space=pltpu.SMEM)
ANY = pl.BlockSpec(memory_space=pl.ANY)


def params(mib):
    return pltpu.CompilerParams(vmem_limit_bytes=mib << 20)


def cost(flops, moved):
    return pl.CostEstimate(flops=flops, bytes_accessed=moved, transcendentals=0)


def terms_kernel(dims, place_ref, heads_ref, weight_ref, far_sent_ref, far_mine_ref, near_sent_ref, near_mine_ref):
    tp, tq, tr, width = dims
    core, here = place_ref[0], place_ref[1]
    span = tr * width
    heads = heads_ref[...]
    for t in range(tp):
        for k, step in enumerate((tq // 2,) + NEAR):
            q = lax.rem(here + (step + tq), tq)
            columns = pl.ds(pl.multiple_of((t * tq + q) * span, span), span)
            terms = jnp.dot(heads, weight_ref[:, columns], preferred_element_type=F32)
            low, high = terms[:, 0:width], terms[:, width:span]
            mine = jnp.where(core == 0, low, high)
            sent = jnp.where(core == 0, high, low).astype(BF16)
            if k == 0:
                far_mine_ref[t] = mine
                far_sent_ref[t] = sent
            else:
                near_mine_ref[k - 1, t] = mine
                near_sent_ref[k - 1, t] = sent


def all_terms(place, heads, weight, dims):
    tp, _, _, width = dims
    tokens, _ = heads.shape
    far, near = (tp, tokens, width), (len(NEAR), tp, tokens, width)
    return pl.pallas_call(
        functools.partial(terms_kernel, dims),
        out_shape=(
            jax.ShapeDtypeStruct(far, BF16),
            jax.ShapeDtypeStruct(far, F32),
            jax.ShapeDtypeStruct(near, BF16),
            jax.ShapeDtypeStruct(near, F32),
        ),
        in_specs=[SMEM, VMEM, VMEM],
        out_specs=(VMEM,) * 4,
        compiler_params=params(16),
        cost_estimate=cost(2 * tokens * weight.size, 2 * weight.size),
        name="all_terms",
    )(place, heads, weight)


def far_kernel(mine_ref, other_ref, right_ref, left_ref):
    half = right_ref.shape[0]
    for k in range(half):
        right_ref[k] = (mine_ref[k] + other_ref[k].astype(F32)).astype(BF16)
        left_ref[k] = (mine_ref[half + k] + other_ref[half + k].astype(F32)).astype(BF16)


def far_block(mine, other):
    half = jax.ShapeDtypeStruct((mine.shape[0] // 2, *mine.shape[1:]), BF16)
    return pl.pallas_call(
        far_kernel,
        out_shape=(half, half),
        in_specs=[VMEM, VMEM],
        out_specs=(VMEM, VMEM),
        compiler_params=params(16),
        cost_estimate=cost(mine.size, 8 * mine.size),
        name="far_block",
    )(mine, other)


def near_kernel(mine_ref, other_ref, left_got_ref, right_got_ref, right_ref, left_ref, own_ref):
    half = left_got_ref.shape[0]
    for t in range(right_ref.shape[0]):
        right = mine_ref[0, t] + other_ref[0, t].astype(F32)
        left = mine_ref[1, t] + other_ref[1, t].astype(F32)
        if t < half:
            right = right + left_got_ref[t].astype(F32)
        else:
            left = left + right_got_ref[t - half].astype(F32)
        right_ref[t] = right.astype(BF16)
        left_ref[t] = left.astype(BF16)
        own_ref[t] = mine_ref[2, t] + other_ref[2, t].astype(F32)


def near_blocks(mine, other, left_got, right_got):
    shape = mine.shape[1:]
    block = jax.ShapeDtypeStruct(shape, BF16)
    return pl.pallas_call(
        near_kernel,
        out_shape=(block, block, jax.ShapeDtypeStruct(shape, F32)),
        in_specs=[VMEM] * 4,
        out_specs=(VMEM, VMEM, VMEM),
        compiler_params=params(16),
        cost_estimate=cost(mine.size, 8 * mine.size),
        name="near_blocks",
    )(mine, other, left_got, right_got)


def summed_kernel(own_ref, left_ref, right_ref, out_ref):
    for t in range(out_ref.shape[0]):
        total = own_ref[t] + left_ref[t].astype(F32) + right_ref[t].astype(F32)
        out_ref[t] = total.astype(BF16)


def summed(own, left, right):
    return pl.pallas_call(
        summed_kernel,
        out_shape=jax.ShapeDtypeStruct(own.shape, BF16),
        in_specs=[VMEM] * 3,
        out_specs=VMEM,
        compiler_params=params(16),
        cost_estimate=cost(2 * own.size, 8 * own.size),
        name="summed",
    )(own, left, right)


def in_three(value):
    first = value.astype(BF16)
    rest = value - first.astype(F32)
    second = rest.astype(BF16)
    third = (rest - second.astype(F32)).astype(BF16)
    return [first.astype(F32), second.astype(F32), third.astype(F32)]


def normed_kernel(parts_ref, residual_ref, gain_ref, hidden_ref, sent_ref):
    total = parts_ref[0].astype(F32)
    for k in range(1, parts_ref.shape[0]):
        total = total + parts_ref[k].astype(F32)
    hidden = (residual_ref[...].astype(F32) + total).astype(BF16)
    hidden_ref[...] = hidden
    widened = hidden.astype(F32)
    gained = widened * gain_ref[...].astype(F32)
    tokens, width = gained.shape
    blank = jnp.zeros((width - tokens, width), F32)

    def turned(rows):
        return jnp.transpose(jnp.concatenate([rows, blank], axis=0))

    squares = jnp.sum(turned(widened * widened), axis=0, keepdims=True)
    top = jnp.max(turned(jnp.abs(gained)), axis=0, keepdims=True)
    lines = in_three(squares) + in_three(top)
    lines.append(jnp.zeros((STAT_ROWS - len(lines), width), F32))
    block = jnp.concatenate([gained] + lines, axis=0).astype(BF16)
    for k in range(sent_ref.shape[0]):
        sent_ref[k] = block


def normed(parts, residual, gain):
    copies, tokens, width = parts.shape
    return pl.pallas_call(
        normed_kernel,
        out_shape=(
            jax.ShapeDtypeStruct((tokens, width), BF16),
            jax.ShapeDtypeStruct((copies, tokens + STAT_ROWS, width), BF16),
        ),
        in_specs=[VMEM, VMEM, VMEM],
        out_specs=(VMEM, VMEM),
        compiler_params=params(16),
        cost_estimate=cost(parts.size, 4 * parts.size),
        name="normed",
    )(parts, residual, gain)


def query_sum(core, dims, tokens, found_ref, weight_ref):
    tp, tq, tr, width = dims
    group = 4
    total = None
    for q in range(tq):
        for t in range(0, tp, group):
            turns = range(t, min(t + group, tp))
            starts = [pl.multiple_of(((k * tq + q) * tr + core) * width, width) for k in turns]
            left = jnp.concatenate(
                [found_ref[q, k * tokens : (k + 1) * tokens, :] for k in turns], axis=1
            )
            right = jnp.concatenate([weight_ref[pl.ds(at, width), :] for at in starts], axis=0)
            term = jnp.dot(left, right, preferred_element_type=F32)
            total = term if total is None else total + term
    return total


def stat_lines(blocks):
    squares, top = None, None
    for block in blocks:
        lines = block.astype(F32)
        found = (lines[0:1] + lines[1:2]) + lines[2:3]
        largest = (lines[3:4] + lines[4:5]) + lines[5:6]
        squares = found if squares is None else squares + found
        top = largest if top is None else jnp.maximum(top, largest)
    return squares, top


def plane_stats(found_ref):
    rows = found_ref.shape[1]
    return stat_lines([found_ref[q, rows - STAT_ROWS :, :] for q in range(found_ref.shape[0])])


def query_half_kernel(dims, core_ref, found_ref, weight_ref, part_ref, stat_ref):
    tokens = part_ref.shape[0]
    part_ref[...] = query_sum(core_ref[0], dims, tokens, found_ref, weight_ref)
    squares, top = plane_stats(found_ref)
    stat_ref[0:1, :] = squares
    stat_ref[1:2, :] = top


def query_half(core, found, weight, dims, tokens):
    width = dims[3]
    return pl.pallas_call(
        functools.partial(query_half_kernel, dims),
        out_shape=(
            jax.ShapeDtypeStruct((tokens, width), F32),
            jax.ShapeDtypeStruct((2, width), F32),
        ),
        in_specs=[SMEM, VMEM, VMEM],
        out_specs=(VMEM, VMEM),
        compiler_params=params(16),
        cost_estimate=cost(tokens * weight.size, weight.size),
        name="query_half",
    )(core, found, weight)


def query_kernel(dims, features, core_ref, part_ref, stat_ref, other_ref, weight_ref, hidden_ref, query_ref, peak_ref, hidden_out_ref):
    tokens, width = query_ref.shape
    hidden_out_ref[...] = hidden_ref[...]
    squares, top = plane_stats(other_ref)
    squares = squares + stat_ref[0:1, :]
    top = jnp.maximum(top, stat_ref[1:2, :])
    inv_rms = lax.rsqrt(squares / features + EPS)
    peak = top * inv_rms
    peak_ref[...] = peak[:, 0:tokens]
    scale = inv_rms * (TOP / (peak + TINY)) * ((peak + TINY) / TOP)
    column = jnp.transpose(jnp.broadcast_to(scale, (width, width)))
    other = query_sum(1 - core_ref[0], dims, tokens, other_ref, weight_ref)
    query_ref[...] = ((part_ref[...] + other) * column[0:tokens, :]).astype(BF16)


def query_rest(core, part, stats, other, weight, hidden, dims, features):
    tokens, width = hidden.shape
    return pl.pallas_call(
        functools.partial(query_kernel, dims, features),
        out_shape=(
            jax.ShapeDtypeStruct((tokens, width), BF16),
            jax.ShapeDtypeStruct((1, tokens), F32),
            jax.ShapeDtypeStruct((tokens, width), BF16),
        ),
        in_specs=[SMEM] + [VMEM] * 5,
        out_specs=(VMEM, VMEM, VMEM),
        compiler_params=params(16),
        cost_estimate=cost(tokens * weight.size, weight.size),
        name="query_rest",
    )(core, part, stats, other, weight, hidden)


def restacked_kernel(line_ref, out_ref):
    tp, rows, width = line_ref.shape
    tokens = rows - STAT_ROWS
    squares, top = stat_lines([line_ref[t, tokens:rows, :] for t in range(tp)])
    lines = in_three(squares) + in_three(top)
    lines.append(jnp.zeros((STAT_ROWS - len(lines), width), F32))
    block = jnp.concatenate(lines, axis=0).astype(BF16)
    for k in range(out_ref.shape[0]):
        for t in range(tp):
            out_ref[k, t * tokens : (t + 1) * tokens, :] = line_ref[t, 0:tokens, :]
        out_ref[k, tp * tokens : tp * tokens + STAT_ROWS, :] = block


def restacked(line, copies):
    tp, rows, width = line.shape
    shape = (copies, tp * (rows - STAT_ROWS) + STAT_ROWS, width)
    return pl.pallas_call(
        restacked_kernel,
        out_shape=jax.ShapeDtypeStruct(shape, BF16),
        in_specs=[VMEM],
        out_specs=VMEM,
        compiler_params=params(16),
        cost_estimate=cost(line.size, 8 * line.size),
        name="restacked",
    )(line)


def exchanged(blocks, axis):
    return lax.all_to_all(blocks, axis, split_axis=0, concat_axis=0, tiled=True)


def swapped(array):
    return lax.ppermute(array, "tr", [(0, 1), (1, 0)])


def moved(array, step):
    size = lax.axis_size("tq")
    return lax.ppermute(array, "tq", [(k, (k + step) % size) for k in range(size)])


def step(attn_heads, residual, o_weight, norm_gain, q_weight):
    tp, tq, tr = (lax.axis_size(axis) for axis in ("tp", "tq", "tr"))
    tokens, width = residual.shape
    features = o_weight.shape[1]
    dims = (tp, tq, tr, width)
    core = lax.axis_index("tr").astype(jnp.int32)
    here = lax.axis_index("tq").astype(jnp.int32)
    place = jnp.stack([core, here])

    far_sent, far_mine, near_sent, near_mine = all_terms(place, attn_heads, o_weight, dims)
    far_right, far_left = far_block(far_mine, swapped(far_sent))
    near_came = swapped(near_sent)
    left_got, right_got = moved(far_right, 1), moved(far_left, -1)
    right, left, own = near_blocks(near_mine, near_came, left_got, right_got)
    section = summed(own, moved(right, 1), moved(left, -1))
    hidden, block = normed(exchanged(section, "tp"), residual, norm_gain.reshape(1, width))

    plane = exchanged(restacked(exchanged(block, "tp"), tq), "tq")
    other_plane = swapped(plane)
    mine_core = core.reshape(1)
    part, stats = query_half(mine_core, plane, q_weight, dims, tokens)
    query, peak, hidden = query_rest(
        mine_core, part, stats, other_plane, q_weight, hidden, dims, features
    )
    return hidden, peak.reshape(tokens), query


def solution(mesh):
    split = ("tp", "tq", "tr")
    placed = (P("groups", split), P("groups", split), P(split, None), P(split), P(None, split))
    return jax.shard_map(
        step,
        mesh=mesh,
        in_specs=placed,
        out_specs=(P("groups", split), P("groups"), P("groups", split)),
        check_vma=False,
    )
```

```python
import functools

import jax
import jax.numpy as jnp
from jax import lax
from jax.experimental import pallas as pl
from jax.experimental.pallas import tpu as pltpu
from jax.sharding import PartitionSpec as P


EPS = 1e-05
TINY = 1e-06
TOP = 448.0
OPENING = 10000000000
BF16, F32 = jnp.bfloat16, jnp.float32
STAT_ROWS = 8
NEAR = (1, -1, 0)
VMEM = pl.BlockSpec(memory_space=pltpu.VMEM)
SMEM = pl.BlockSpec(memory_space=pltpu.SMEM)
ANY = pl.BlockSpec(memory_space=pl.ANY)


def params(mib):
    return pltpu.CompilerParams(vmem_limit_bytes=mib << 20)


def cost(flops, moved):
    return pl.CostEstimate(flops=flops, bytes_accessed=moved, transcendentals=0)


def opening_kernel(place_ref, out_ref):
    out_ref[...] = jnp.zeros_like(out_ref) + place_ref[0].astype(F32)


def opening(place):
    return pl.pallas_call(
        opening_kernel,
        out_shape=jax.ShapeDtypeStruct((8, 128), F32),
        in_specs=[SMEM],
        out_specs=VMEM,
        compiler_params=params(16),
        cost_estimate=cost(OPENING, OPENING),
        name="opening",
    )(place)


def terms_kernel(dims, place_ref, heads_ref, weight_ref, after_ref, far_sent_ref, far_mine_ref, near_sent_ref, near_mine_ref):
    tp, tq, tr, width = dims
    core, here = place_ref[0], place_ref[1]
    span = tr * width
    heads = heads_ref[...]
    for t in range(tp):
        for k, step in enumerate((tq // 2,) + NEAR):
            q = lax.rem(here + (step + tq), tq)
            columns = pl.ds(pl.multiple_of((t * tq + q) * span, span), span)
            terms = jnp.dot(heads, weight_ref[:, columns], preferred_element_type=F32)
            low, high = terms[:, 0:width], terms[:, width:span]
            mine = jnp.where(core == 0, low, high)
            sent = jnp.where(core == 0, high, low).astype(BF16)
            if k == 0:
                far_mine_ref[t] = mine
                far_sent_ref[t] = sent
            else:
                near_mine_ref[k - 1, t] = mine
                near_sent_ref[k - 1, t] = sent


def all_terms(place, heads, weight, after, dims):
    tp, _, _, width = dims
    tokens, _ = heads.shape
    far, near = (tp, tokens, width), (len(NEAR), tp, tokens, width)
    return pl.pallas_call(
        functools.partial(terms_kernel, dims),
        out_shape=(
            jax.ShapeDtypeStruct(far, BF16),
            jax.ShapeDtypeStruct(far, F32),
            jax.ShapeDtypeStruct(near, BF16),
            jax.ShapeDtypeStruct(near, F32),
        ),
        in_specs=[SMEM, VMEM, VMEM, ANY],
        out_specs=(VMEM,) * 4,
        compiler_params=params(16),
        cost_estimate=cost(2 * tokens * weight.size, 2 * weight.size),
        name="all_terms",
    )(place, heads, weight, after)


def far_kernel(mine_ref, other_ref, right_ref, left_ref):
    half = right_ref.shape[0]
    for k in range(half):
        right_ref[k] = (mine_ref[k] + other_ref[k].astype(F32)).astype(BF16)
        left_ref[k] = (mine_ref[half + k] + other_ref[half + k].astype(F32)).astype(BF16)


def far_block(mine, other):
    half = jax.ShapeDtypeStruct((mine.shape[0] // 2, *mine.shape[1:]), BF16)
    return pl.pallas_call(
        far_kernel,
        out_shape=(half, half),
        in_specs=[VMEM, VMEM],
        out_specs=(VMEM, VMEM),
        compiler_params=params(16),
        cost_estimate=cost(mine.size, 8 * mine.size),
        name="far_block",
    )(mine, other)


def near_kernel(mine_ref, other_ref, left_got_ref, right_got_ref, right_ref, left_ref, own_ref):
    half = left_got_ref.shape[0]
    for t in range(right_ref.shape[0]):
        right = mine_ref[0, t] + other_ref[0, t].astype(F32)
        left = mine_ref[1, t] + other_ref[1, t].astype(F32)
        if t < half:
            right = right + left_got_ref[t].astype(F32)
        else:
            left = left + right_got_ref[t - half].astype(F32)
        right_ref[t] = right.astype(BF16)
        left_ref[t] = left.astype(BF16)
        own_ref[t] = mine_ref[2, t] + other_ref[2, t].astype(F32)


def near_blocks(mine, other, left_got, right_got):
    shape = mine.shape[1:]
    block = jax.ShapeDtypeStruct(shape, BF16)
    return pl.pallas_call(
        near_kernel,
        out_shape=(block, block, jax.ShapeDtypeStruct(shape, F32)),
        in_specs=[VMEM] * 4,
        out_specs=(VMEM, VMEM, VMEM),
        compiler_params=params(16),
        cost_estimate=cost(mine.size, 8 * mine.size),
        name="near_blocks",
    )(mine, other, left_got, right_got)


def summed_kernel(own_ref, left_ref, right_ref, out_ref):
    for t in range(out_ref.shape[0]):
        total = own_ref[t] + left_ref[t].astype(F32) + right_ref[t].astype(F32)
        out_ref[t] = total.astype(BF16)


def summed(own, left, right):
    return pl.pallas_call(
        summed_kernel,
        out_shape=jax.ShapeDtypeStruct(own.shape, BF16),
        in_specs=[VMEM] * 3,
        out_specs=VMEM,
        compiler_params=params(16),
        cost_estimate=cost(2 * own.size, 8 * own.size),
        name="summed",
    )(own, left, right)


def in_three(value):
    first = value.astype(BF16)
    rest = value - first.astype(F32)
    second = rest.astype(BF16)
    third = (rest - second.astype(F32)).astype(BF16)
    return [first.astype(F32), second.astype(F32), third.astype(F32)]


def normed_kernel(parts_ref, residual_ref, gain_ref, hidden_ref, sent_ref):
    total = parts_ref[0].astype(F32)
    for k in range(1, parts_ref.shape[0]):
        total = total + parts_ref[k].astype(F32)
    hidden = (residual_ref[...].astype(F32) + total).astype(BF16)
    hidden_ref[...] = hidden
    widened = hidden.astype(F32)
    gained = widened * gain_ref[...].astype(F32)
    tokens, width = gained.shape
    blank = jnp.zeros((width - tokens, width), F32)

    def turned(rows):
        return jnp.transpose(jnp.concatenate([rows, blank], axis=0))

    squares = jnp.sum(turned(widened * widened), axis=0, keepdims=True)
    top = jnp.max(turned(jnp.abs(gained)), axis=0, keepdims=True)
    lines = in_three(squares) + in_three(top)
    lines.append(jnp.zeros((STAT_ROWS - len(lines), width), F32))
    block = jnp.concatenate([gained] + lines, axis=0).astype(BF16)
    for k in range(sent_ref.shape[0]):
        sent_ref[k] = block


def normed(parts, residual, gain):
    copies, tokens, width = parts.shape
    return pl.pallas_call(
        normed_kernel,
        out_shape=(
            jax.ShapeDtypeStruct((tokens, width), BF16),
            jax.ShapeDtypeStruct((copies, tokens + STAT_ROWS, width), BF16),
        ),
        in_specs=[VMEM, VMEM, VMEM],
        out_specs=(VMEM, VMEM),
        compiler_params=params(16),
        cost_estimate=cost(parts.size, 4 * parts.size),
        name="normed",
    )(parts, residual, gain)


def query_sum(core, dims, tokens, found_ref, weight_ref):
    tp, tq, tr, width = dims
    group = 4
    total = None
    for q in range(tq):
        for t in range(0, tp, group):
            turns = range(t, min(t + group, tp))
            starts = [pl.multiple_of(((k * tq + q) * tr + core) * width, width) for k in turns]
            left = jnp.concatenate(
                [found_ref[q, k * tokens : (k + 1) * tokens, :] for k in turns], axis=1
            )
            right = jnp.concatenate([weight_ref[pl.ds(at, width), :] for at in starts], axis=0)
            term = jnp.dot(left, right, preferred_element_type=F32)
            total = term if total is None else total + term
    return total


def stat_lines(blocks):
    squares, top = None, None
    for block in blocks:
        lines = block.astype(F32)
        found = (lines[0:1] + lines[1:2]) + lines[2:3]
        largest = (lines[3:4] + lines[4:5]) + lines[5:6]
        squares = found if squares is None else squares + found
        top = largest if top is None else jnp.maximum(top, largest)
    return squares, top


def plane_stats(found_ref):
    rows = found_ref.shape[1]
    return stat_lines([found_ref[q, rows - STAT_ROWS :, :] for q in range(found_ref.shape[0])])


def query_half_kernel(dims, core_ref, found_ref, weight_ref, part_ref, stat_ref):
    tokens = part_ref.shape[0]
    part_ref[...] = query_sum(core_ref[0], dims, tokens, found_ref, weight_ref)
    squares, top = plane_stats(found_ref)
    stat_ref[0:1, :] = squares
    stat_ref[1:2, :] = top


def query_half(core, found, weight, dims, tokens):
    width = dims[3]
    return pl.pallas_call(
        functools.partial(query_half_kernel, dims),
        out_shape=(
            jax.ShapeDtypeStruct((tokens, width), F32),
            jax.ShapeDtypeStruct((2, width), F32),
        ),
        in_specs=[SMEM, VMEM, VMEM],
        out_specs=(VMEM, VMEM),
        compiler_params=params(16),
        cost_estimate=cost(tokens * weight.size, weight.size),
        name="query_half",
    )(core, found, weight)


def query_kernel(dims, features, core_ref, part_ref, stat_ref, other_ref, weight_ref, hidden_ref, query_ref, peak_ref, hidden_out_ref):
    tokens, width = query_ref.shape
    hidden_out_ref[...] = hidden_ref[...]
    squares, top = plane_stats(other_ref)
    squares = squares + stat_ref[0:1, :]
    top = jnp.maximum(top, stat_ref[1:2, :])
    inv_rms = lax.rsqrt(squares / features + EPS)
    peak = top * inv_rms
    peak_ref[...] = peak[:, 0:tokens]
    scale = inv_rms * (TOP / (peak + TINY)) * ((peak + TINY) / TOP)
    column = jnp.transpose(jnp.broadcast_to(scale, (width, width)))
    other = query_sum(1 - core_ref[0], dims, tokens, other_ref, weight_ref)
    query_ref[...] = ((part_ref[...] + other) * column[0:tokens, :]).astype(BF16)


def query_rest(core, part, stats, other, weight, hidden, dims, features):
    tokens, width = hidden.shape
    return pl.pallas_call(
        functools.partial(query_kernel, dims, features),
        out_shape=(
            jax.ShapeDtypeStruct((tokens, width), BF16),
            jax.ShapeDtypeStruct((1, tokens), F32),
            jax.ShapeDtypeStruct((tokens, width), BF16),
        ),
        in_specs=[SMEM] + [VMEM] * 5,
        out_specs=(VMEM, VMEM, VMEM),
        compiler_params=params(16),
        cost_estimate=cost(tokens * weight.size, weight.size),
        name="query_rest",
    )(core, part, stats, other, weight, hidden)


def restacked_kernel(line_ref, out_ref):
    tp, rows, width = line_ref.shape
    tokens = rows - STAT_ROWS
    squares, top = stat_lines([line_ref[t, tokens:rows, :] for t in range(tp)])
    lines = in_three(squares) + in_three(top)
    lines.append(jnp.zeros((STAT_ROWS - len(lines), width), F32))
    block = jnp.concatenate(lines, axis=0).astype(BF16)
    for k in range(out_ref.shape[0]):
        for t in range(tp):
            out_ref[k, t * tokens : (t + 1) * tokens, :] = line_ref[t, 0:tokens, :]
        out_ref[k, tp * tokens : tp * tokens + STAT_ROWS, :] = block


def restacked(line, copies):
    tp, rows, width = line.shape
    shape = (copies, tp * (rows - STAT_ROWS) + STAT_ROWS, width)
    return pl.pallas_call(
        restacked_kernel,
        out_shape=jax.ShapeDtypeStruct(shape, BF16),
        in_specs=[VMEM],
        out_specs=VMEM,
        compiler_params=params(16),
        cost_estimate=cost(line.size, 8 * line.size),
        name="restacked",
    )(line)


def exchanged(blocks, axis):
    return lax.all_to_all(blocks, axis, split_axis=0, concat_axis=0, tiled=True)


def swapped(array):
    return lax.ppermute(array, "tr", [(0, 1), (1, 0)])


def moved(array, step):
    size = lax.axis_size("tq")
    return lax.ppermute(array, "tq", [(k, (k + step) % size) for k in range(size)])


def step(attn_heads, residual, o_weight, norm_gain, q_weight):
    tp, tq, tr = (lax.axis_size(axis) for axis in ("tp", "tq", "tr"))
    tokens, width = residual.shape
    features = o_weight.shape[1]
    dims = (tp, tq, tr, width)
    core = lax.axis_index("tr").astype(jnp.int32)
    here = lax.axis_index("tq").astype(jnp.int32)
    place = jnp.stack([core, here])

    far_sent, far_mine, near_sent, near_mine = all_terms(
        place, attn_heads, o_weight, opening(place), dims
    )
    far_right, far_left = far_block(far_mine, swapped(far_sent))
    near_came = swapped(near_sent)
    left_got, right_got = moved(far_right, 1), moved(far_left, -1)
    right, left, own = near_blocks(near_mine, near_came, left_got, right_got)
    section = summed(own, moved(right, 1), moved(left, -1))
    hidden, block = normed(exchanged(section, "tp"), residual, norm_gain.reshape(1, width))

    plane = exchanged(restacked(exchanged(block, "tp"), tq), "tq")
    other_plane = swapped(plane)
    mine_core = core.reshape(1)
    part, stats = query_half(mine_core, plane, q_weight, dims, tokens)
    query, peak, hidden = query_rest(
        mine_core, part, stats, other_plane, q_weight, hidden, dims, features
    )
    return hidden, peak.reshape(tokens), query


def solution(mesh):
    split = ("tp", "tq", "tr")
    placed = (P("groups", split), P("groups", split), P(split, None), P(split), P(None, split))
    return jax.shard_map(
        step,
        mesh=mesh,
        in_specs=placed,
        out_specs=(P("groups", split), P("groups"), P("groups", split)),
        check_vma=False,
    )
```

```python
import functools

import jax
import jax.numpy as jnp
from jax import lax
from jax.experimental import pallas as pl
from jax.experimental.pallas import tpu as pltpu
from jax.sharding import PartitionSpec as P


EPS = 1e-05
TINY = 1e-06
TOP = 448.0
OPENING = 10000000000
BF16, F32 = jnp.bfloat16, jnp.float32
STAT_ROWS = 8
NEAR = (1, -1, 0)
VMEM = pl.BlockSpec(memory_space=pltpu.VMEM)
SMEM = pl.BlockSpec(memory_space=pltpu.SMEM)
ANY = pl.BlockSpec(memory_space=pl.ANY)


def params(mib):
    return pltpu.CompilerParams(vmem_limit_bytes=mib << 20)


def cost(flops, moved):
    return pl.CostEstimate(flops=flops, bytes_accessed=moved, transcendentals=0)


def opening_kernel(place_ref, out_ref):
    out_ref[...] = jnp.zeros_like(out_ref) + place_ref[0].astype(F32)


def opening(place):
    return pl.pallas_call(
        opening_kernel,
        out_shape=jax.ShapeDtypeStruct((8, 128), F32),
        in_specs=[SMEM],
        out_specs=VMEM,
        compiler_params=params(16),
        cost_estimate=cost(OPENING, OPENING),
        name="opening",
    )(place)


def terms_kernel(dims, steps, place_ref, heads_ref, weight_ref, after_ref, sent_ref, mine_ref):
    tp, tq, tr, width = dims
    core, here = place_ref[0], place_ref[1]
    span = tr * width
    heads = heads_ref[...]
    for t in range(tp):
        for k, step in enumerate(steps):
            q = lax.rem(here + (step + tq), tq)
            columns = pl.ds(pl.multiple_of((t * tq + q) * span, span), span)
            terms = jnp.dot(heads, weight_ref[:, columns], preferred_element_type=F32)
            low, high = terms[:, 0:width], terms[:, width:span]
            mine_ref[k, t] = jnp.where(core == 0, low, high)
            sent_ref[k, t] = jnp.where(core == 0, high, low).astype(BF16)


def some_terms(place, heads, weight, after, dims, steps):
    tp, _, _, width = dims
    tokens, _ = heads.shape
    shape = (len(steps), tp, tokens, width)
    return pl.pallas_call(
        functools.partial(terms_kernel, dims, steps),
        out_shape=(jax.ShapeDtypeStruct(shape, BF16), jax.ShapeDtypeStruct(shape, F32)),
        in_specs=[SMEM, VMEM, VMEM, ANY],
        out_specs=(VMEM,) * 2,
        compiler_params=params(16),
        cost_estimate=cost(2 * tokens * weight.size, 2 * weight.size),
        name="some_terms",
    )(place, heads, weight, after)


def far_kernel(mine_ref, other_ref, right_ref, left_ref):
    half = right_ref.shape[0]
    for k in range(half):
        right_ref[k] = (mine_ref[k] + other_ref[k].astype(F32)).astype(BF16)
        left_ref[k] = (mine_ref[half + k] + other_ref[half + k].astype(F32)).astype(BF16)


def far_block(mine, other):
    half = jax.ShapeDtypeStruct((mine.shape[0] // 2, *mine.shape[1:]), BF16)
    return pl.pallas_call(
        far_kernel,
        out_shape=(half, half),
        in_specs=[VMEM, VMEM],
        out_specs=(VMEM, VMEM),
        compiler_params=params(16),
        cost_estimate=cost(mine.size, 8 * mine.size),
        name="far_block",
    )(mine, other)


def near_kernel(mine_ref, other_ref, left_got_ref, right_got_ref, right_ref, left_ref, own_ref):
    half = left_got_ref.shape[0]
    for t in range(right_ref.shape[0]):
        right = mine_ref[0, t] + other_ref[0, t].astype(F32)
        left = mine_ref[1, t] + other_ref[1, t].astype(F32)
        if t < half:
            right = right + left_got_ref[t].astype(F32)
        else:
            left = left + right_got_ref[t - half].astype(F32)
        right_ref[t] = right.astype(BF16)
        left_ref[t] = left.astype(BF16)
        own_ref[t] = mine_ref[2, t] + other_ref[2, t].astype(F32)


def near_blocks(mine, other, left_got, right_got):
    shape = mine.shape[1:]
    block = jax.ShapeDtypeStruct(shape, BF16)
    return pl.pallas_call(
        near_kernel,
        out_shape=(block, block, jax.ShapeDtypeStruct(shape, F32)),
        in_specs=[VMEM] * 4,
        out_specs=(VMEM, VMEM, VMEM),
        compiler_params=params(16),
        cost_estimate=cost(mine.size, 8 * mine.size),
        name="near_blocks",
    )(mine, other, left_got, right_got)


def summed_kernel(own_ref, left_ref, right_ref, out_ref):
    for t in range(out_ref.shape[0]):
        total = own_ref[t] + left_ref[t].astype(F32) + right_ref[t].astype(F32)
        out_ref[t] = total.astype(BF16)


def summed(own, left, right):
    return pl.pallas_call(
        summed_kernel,
        out_shape=jax.ShapeDtypeStruct(own.shape, BF16),
        in_specs=[VMEM] * 3,
        out_specs=VMEM,
        compiler_params=params(16),
        cost_estimate=cost(2 * own.size, 8 * own.size),
        name="summed",
    )(own, left, right)


def in_three(value):
    first = value.astype(BF16)
    rest = value - first.astype(F32)
    second = rest.astype(BF16)
    third = (rest - second.astype(F32)).astype(BF16)
    return [first.astype(F32), second.astype(F32), third.astype(F32)]


def normed_kernel(parts_ref, residual_ref, gain_ref, hidden_ref, sent_ref):
    total = parts_ref[0].astype(F32)
    for k in range(1, parts_ref.shape[0]):
        total = total + parts_ref[k].astype(F32)
    hidden = (residual_ref[...].astype(F32) + total).astype(BF16)
    hidden_ref[...] = hidden
    widened = hidden.astype(F32)
    gained = widened * gain_ref[...].astype(F32)
    tokens, width = gained.shape
    blank = jnp.zeros((width - tokens, width), F32)

    def turned(rows):
        return jnp.transpose(jnp.concatenate([rows, blank], axis=0))

    squares = jnp.sum(turned(widened * widened), axis=0, keepdims=True)
    top = jnp.max(turned(jnp.abs(gained)), axis=0, keepdims=True)
    lines = in_three(squares) + in_three(top)
    lines.append(jnp.zeros((STAT_ROWS - len(lines), width), F32))
    block = jnp.concatenate([gained] + lines, axis=0).astype(BF16)
    for k in range(sent_ref.shape[0]):
        sent_ref[k] = block


def normed(parts, residual, gain):
    copies, tokens, width = parts.shape
    return pl.pallas_call(
        normed_kernel,
        out_shape=(
            jax.ShapeDtypeStruct((tokens, width), BF16),
            jax.ShapeDtypeStruct((copies, tokens + STAT_ROWS, width), BF16),
        ),
        in_specs=[VMEM, VMEM, VMEM],
        out_specs=(VMEM, VMEM),
        compiler_params=params(16),
        cost_estimate=cost(parts.size, 4 * parts.size),
        name="normed",
    )(parts, residual, gain)


def query_sum(core, dims, tokens, found_ref, weight_ref):
    tp, tq, tr, width = dims
    group = 4
    total = None
    for q in range(tq):
        for t in range(0, tp, group):
            turns = range(t, min(t + group, tp))
            starts = [pl.multiple_of(((k * tq + q) * tr + core) * width, width) for k in turns]
            left = jnp.concatenate(
                [found_ref[q, k * tokens : (k + 1) * tokens, :] for k in turns], axis=1
            )
            right = jnp.concatenate([weight_ref[pl.ds(at, width), :] for at in starts], axis=0)
            term = jnp.dot(left, right, preferred_element_type=F32)
            total = term if total is None else total + term
    return total


def stat_lines(blocks):
    squares, top = None, None
    for block in blocks:
        lines = block.astype(F32)
        found = (lines[0:1] + lines[1:2]) + lines[2:3]
        largest = (lines[3:4] + lines[4:5]) + lines[5:6]
        squares = found if squares is None else squares + found
        top = largest if top is None else jnp.maximum(top, largest)
    return squares, top


def plane_stats(found_ref):
    rows = found_ref.shape[1]
    return stat_lines([found_ref[q, rows - STAT_ROWS :, :] for q in range(found_ref.shape[0])])


def query_half_kernel(dims, core_ref, found_ref, weight_ref, part_ref, stat_ref):
    tokens = part_ref.shape[0]
    part_ref[...] = query_sum(core_ref[0], dims, tokens, found_ref, weight_ref)
    squares, top = plane_stats(found_ref)
    stat_ref[0:1, :] = squares
    stat_ref[1:2, :] = top


def query_half(core, found, weight, dims, tokens):
    width = dims[3]
    return pl.pallas_call(
        functools.partial(query_half_kernel, dims),
        out_shape=(
            jax.ShapeDtypeStruct((tokens, width), F32),
            jax.ShapeDtypeStruct((2, width), F32),
        ),
        in_specs=[SMEM, VMEM, VMEM],
        out_specs=(VMEM, VMEM),
        compiler_params=params(16),
        cost_estimate=cost(tokens * weight.size, weight.size),
        name="query_half",
    )(core, found, weight)


def query_kernel(dims, features, core_ref, part_ref, stat_ref, other_ref, weight_ref, hidden_ref, query_ref, peak_ref, hidden_out_ref):
    tokens, width = query_ref.shape
    hidden_out_ref[...] = hidden_ref[...]
    squares, top = plane_stats(other_ref)
    squares = squares + stat_ref[0:1, :]
    top = jnp.maximum(top, stat_ref[1:2, :])
    inv_rms = lax.rsqrt(squares / features + EPS)
    peak = top * inv_rms
    peak_ref[...] = peak[:, 0:tokens]
    scale = inv_rms * (TOP / (peak + TINY)) * ((peak + TINY) / TOP)
    column = jnp.transpose(jnp.broadcast_to(scale, (width, width)))
    other = query_sum(1 - core_ref[0], dims, tokens, other_ref, weight_ref)
    query_ref[...] = ((part_ref[...] + other) * column[0:tokens, :]).astype(BF16)


def query_rest(core, part, stats, other, weight, hidden, dims, features):
    tokens, width = hidden.shape
    return pl.pallas_call(
        functools.partial(query_kernel, dims, features),
        out_shape=(
            jax.ShapeDtypeStruct((tokens, width), BF16),
            jax.ShapeDtypeStruct((1, tokens), F32),
            jax.ShapeDtypeStruct((tokens, width), BF16),
        ),
        in_specs=[SMEM] + [VMEM] * 5,
        out_specs=(VMEM, VMEM, VMEM),
        compiler_params=params(16),
        cost_estimate=cost(tokens * weight.size, weight.size),
        name="query_rest",
    )(core, part, stats, other, weight, hidden)


def restacked_kernel(line_ref, out_ref):
    tp, rows, width = line_ref.shape
    tokens = rows - STAT_ROWS
    squares, top = stat_lines([line_ref[t, tokens:rows, :] for t in range(tp)])
    lines = in_three(squares) + in_three(top)
    lines.append(jnp.zeros((STAT_ROWS - len(lines), width), F32))
    block = jnp.concatenate(lines, axis=0).astype(BF16)
    for k in range(out_ref.shape[0]):
        for t in range(tp):
            out_ref[k, t * tokens : (t + 1) * tokens, :] = line_ref[t, 0:tokens, :]
        out_ref[k, tp * tokens : tp * tokens + STAT_ROWS, :] = block


def restacked(line, copies):
    tp, rows, width = line.shape
    shape = (copies, tp * (rows - STAT_ROWS) + STAT_ROWS, width)
    return pl.pallas_call(
        restacked_kernel,
        out_shape=jax.ShapeDtypeStruct(shape, BF16),
        in_specs=[VMEM],
        out_specs=VMEM,
        compiler_params=params(16),
        cost_estimate=cost(line.size, 8 * line.size),
        name="restacked",
    )(line)


def exchanged(blocks, axis):
    return lax.all_to_all(blocks, axis, split_axis=0, concat_axis=0, tiled=True)


def swapped(array):
    return lax.ppermute(array, "tr", [(0, 1), (1, 0)])


def moved(array, step):
    size = lax.axis_size("tq")
    return lax.ppermute(array, "tq", [(k, (k + step) % size) for k in range(size)])


def step(attn_heads, residual, o_weight, norm_gain, q_weight):
    tp, tq, tr = (lax.axis_size(axis) for axis in ("tp", "tq", "tr"))
    tokens, width = residual.shape
    features = o_weight.shape[1]
    dims = (tp, tq, tr, width)
    core = lax.axis_index("tr").astype(jnp.int32)
    here = lax.axis_index("tq").astype(jnp.int32)
    place = jnp.stack([core, here])

    first = opening(place)
    far_sent, far_mine = some_terms(place, attn_heads, o_weight, first, dims, (tq // 2,))
    far_sent, far_mine = far_sent[0], far_mine[0]
    near_sent, near_mine = some_terms(place, attn_heads, o_weight, far_mine, dims, NEAR)
    far_right, far_left = far_block(far_mine, swapped(far_sent))
    near_came = swapped(near_sent)
    left_got, right_got = moved(far_right, 1), moved(far_left, -1)
    right, left, own = near_blocks(near_mine, near_came, left_got, right_got)
    section = summed(own, moved(right, 1), moved(left, -1))
    hidden, block = normed(exchanged(section, "tp"), residual, norm_gain.reshape(1, width))

    plane = exchanged(restacked(exchanged(block, "tp"), tq), "tq")
    other_plane = swapped(plane)
    mine_core = core.reshape(1)
    part, stats = query_half(mine_core, plane, q_weight, dims, tokens)
    query, peak, hidden = query_rest(
        mine_core, part, stats, other_plane, q_weight, hidden, dims, features
    )
    return hidden, peak.reshape(tokens), query


def solution(mesh):
    split = ("tp", "tq", "tr")
    placed = (P("groups", split), P("groups", split), P(split, None), P(split), P(None, split))
    return jax.shard_map(
        step,
        mesh=mesh,
        in_specs=placed,
        out_specs=(P("groups", split), P("groups"), P("groups", split)),
        check_vma=False,
    )
```
